32 devices in a mesh: dp: 4 (over y, z), sp: 8 (over x, core).
Axes of the slice: x: 4, y: 2, z: 2, core: 2. Of those that a mesh axis runs over, the one named last changes fastest.
The devices are a block of a 4x4x8 slice.
Arguments:
- x_in: bfloat16 [4, 3072, 2048], P('dp', 'sp'), parts along dimension 0
- d_out: bfloat16 [4, 3072, 2048], P('dp', 'sp'), parts along dimension 0
- gain: float32 [2048], replicated
- w_q: bfloat16 [2048, 32, 64], replicated
- w_k: bfloat16 [2048, 8, 64], replicated
- w_v: bfloat16 [2048, 8, 64], replicated
- w_o: bfloat16 [32, 64, 2048], replicated
Outputs:
- output 1: bfloat16 [4, 3072, 2048], P('dp', 'sp'), parts along dimension 0
- output 2: bfloat16 [4, 3072, 2048], P('dp', 'sp'), parts along dimension 0
- output 3: float32 [8192, 32, 64], P('dp'), parts along dimension 0
- output 4: float32 [8192, 8, 64], P('dp'), parts along dimension 0
- output 5: float32 [8192, 8, 64], P('dp'), parts along dimension 0
- output 6: float32 [128, 64, 2048], P('dp'), parts along dimension 0
- output 7: float32 [8192], P('dp'), parts along dimension 0
There are 4 independent parts. The reference program is written for one: setup_inputs(seed, part) draws one part's arguments, and reference() takes and returns one part's arrays. A program takes and returns all parts, laid end to end along the dimension named above; an argument that names none is the same for every part.
All inputs are finite; a program needn't handle non-finite values.
Results may differ from the reference program's by a relative error of at most 0.0122979.
Values are sent between devices in bfloat16 or wider.
A program may use at most 768 MiB of HBM per device.

```python
import jax
import jax.numpy as jnp
from jax import lax

BATCH = 1
SEQ = 3072
D_MODEL = 2048
HEADS = 32
KV_HEADS = 8
HEAD = 64

ROPE_BASE = 1000000.0
NORM_EPS = 1e-5


def setup_inputs(seed: int = 0, part: int = 0) -> dict:
    part_key = jax.random.fold_in(jax.random.key(seed), part)
    key_x, key_dy = jax.random.split(part_key, 2)
    shared = jax.random.split(jax.random.key(seed + 1), 5)
    x_val = jax.random.normal(key_x, (BATCH, SEQ, D_MODEL), jnp.float32)
    dy_val = jax.random.normal(key_dy, (BATCH, SEQ, D_MODEL), jnp.float32)
    gain = jax.random.uniform(shared[0], (D_MODEL,), jnp.float32, 0.6, 1.4)
    in_scale = D_MODEL ** -0.5
    w_q = jax.random.normal(shared[1], (D_MODEL, HEADS, HEAD), jnp.float32) * (1.5 * in_scale)
    w_k = jax.random.normal(shared[2], (D_MODEL, KV_HEADS, HEAD), jnp.float32) * (1.5 * in_scale)
    w_v = jax.random.normal(shared[3], (D_MODEL, KV_HEADS, HEAD), jnp.float32) * in_scale
    w_o = jax.random.normal(shared[4], (HEADS, HEAD, D_MODEL), jnp.float32) * (2.0 * (HEADS * HEAD) ** -0.5)
    return {'x_in': x_val.astype(jnp.bfloat16), 'd_out': dy_val.astype(jnp.bfloat16), 'gain': gain, 'w_q': w_q.astype(jnp.bfloat16), 'w_k': w_k.astype(jnp.bfloat16), 'w_v': w_v.astype(jnp.bfloat16), 'w_o': w_o.astype(jnp.bfloat16)}


def rope_tables(positions):
    half = HEAD // 2
    inv_freq = ROPE_BASE ** (-2.0 * jnp.arange(half, dtype=jnp.float32) / HEAD)
    angle = positions[:, None] * inv_freq[None, :]
    return jnp.cos(angle), jnp.sin(angle)


def rotate(t_val, cos_t, sin_t):
    half = HEAD // 2
    first = t_val[..., :half]
    second = t_val[..., half:]
    cos_b = cos_t[:, None, :]
    sin_b = sin_t[:, None, :]
    return jnp.concatenate([first * cos_b - second * sin_b, second * cos_b + first * sin_b], axis=-1)


def attention(q_all, k_all, v_all):
    group = HEADS // KV_HEADS
    block_len = 128
    num_blocks = SEQ // block_len
    scale = HEAD ** -0.5
    k_f32 = k_all.astype(jnp.float32)
    v_f32 = v_all.astype(jnp.float32)
    q_grouped = jnp.moveaxis(q_all.reshape(BATCH, num_blocks, block_len, KV_HEADS, group, HEAD), 1, 0)
    key_pos = jnp.arange(SEQ)

    def one_block(pair):
        q_rows, block_idx = pair
        scores = jnp.einsum('bqkgd,btkd->bkgqt', q_rows.astype(jnp.float32), k_f32) * scale
        q_pos = block_idx * block_len + jnp.arange(block_len)
        scores = jnp.where(key_pos[None, :] <= q_pos[:, None], scores, -1e30)
        attn_weights = jax.nn.softmax(scores, axis=-1).astype(jnp.bfloat16).astype(jnp.float32)
        out_rows = jnp.einsum('bkgqt,btkd->bqkgd', attn_weights, v_f32)
        return out_rows.astype(jnp.bfloat16)

    out_blocks = lax.map(jax.checkpoint(one_block), (q_grouped, jnp.arange(num_blocks)))
    return jnp.moveaxis(out_blocks, 0, 1).reshape(BATCH, SEQ, HEADS, HEAD)


def block_forward(x_in, gain, w_q, w_k, w_v, w_o):
    x_f32 = x_in.astype(jnp.float32)
    inv_rms = lax.rsqrt(jnp.mean(x_f32 * x_f32, axis=-1, keepdims=True) + NORM_EPS)
    normed = (x_f32 * inv_rms * gain).astype(jnp.bfloat16).astype(jnp.float32)
    cos_t, sin_t = rope_tables(jnp.arange(SEQ, dtype=jnp.float32))
    q_all = rotate(jnp.einsum('btd,dhe->bthe', normed, w_q), cos_t, sin_t).astype(jnp.bfloat16)
    k_all = rotate(jnp.einsum('btd,dhe->bthe', normed, w_k), cos_t, sin_t).astype(jnp.bfloat16)
    v_all = jnp.einsum('btd,dhe->bthe', normed, w_v).astype(jnp.bfloat16)
    mixed = attention(q_all, k_all, v_all)
    y_proj = jnp.einsum('bthe,hed->btd', mixed.astype(jnp.float32), w_o)
    return (x_f32 + y_proj).astype(jnp.bfloat16)


def reference(x_in, d_out, gain, w_q, w_k, w_v, w_o):
    y_out, pullback = jax.vjp(block_forward, x_in, gain, w_q.astype(jnp.float32), w_k.astype(jnp.float32), w_v.astype(jnp.float32), w_o.astype(jnp.float32))
    d_x, d_gain, d_wq, d_wk, d_wv, d_wo = pullback(d_out)
    return (y_out, d_x, d_wq, d_wk, d_wv, d_wo, d_gain)
```

```python
import functools
import math
import jax
import jax.numpy as jnp
from jax import lax
from jax.experimental import pallas as pl
from jax.experimental.pallas import tpu as pltpu
from jax.sharding import PartitionSpec as P

ROPE_BASE = 1000000.0
NORM_EPS = 1e-5
LOG2E = math.log2(math.e)
BQ = 256
BK = 256
NT = (((1,), (1,)), ((), ()))
TN = (((0,), (0,)), ((), ()))
F32 = jnp.float32
BF16 = jnp.bfloat16


def rope_tables(positions, head_dim):
    half = head_dim // 2
    inv_freq = ROPE_BASE ** (-2.0 * jnp.arange(half, dtype=F32) / head_dim)
    angle = inv_freq[:, None] * positions[None, :]
    return jnp.cos(angle), jnp.sin(angle)


def rotate(vals, cos_t, sin_t):
    half = vals.shape[-2] // 2
    first = vals[..., :half, :]
    second = vals[..., half:, :]
    return jnp.concatenate([first * cos_t - second * sin_t, second * cos_t + first * sin_t], axis=-2)


def rotate_back(vals, cos_t, sin_t):
    half = vals.shape[-2] // 2
    first = vals[..., :half, :]
    second = vals[..., half:, :]
    return jnp.concatenate([first * cos_t + second * sin_t, second * cos_t - first * sin_t], axis=-2)


def norm_forward(x_local, gain):
    x_f32 = x_local.astype(F32)
    inv_rms = lax.rsqrt(jnp.mean(x_f32 * x_f32, axis=-1, keepdims=True) + NORM_EPS)
    x_hat = x_f32 * inv_rms
    return x_hat, inv_rms, (x_hat * gain).astype(BF16)


def dot(a, b):
    return jnp.dot(a, b, preferred_element_type=F32)


def dot_nt(a, b):
    return lax.dot_general(a, b, NT, preferred_element_type=F32)


def heads_cat(ref, num):
    dim = ref.shape[0] // num
    return jnp.concatenate([ref[h * dim:(h + 1) * dim, :] for h in range(num)], axis=1)


class RingGather:
    def __init__(self, seq_par, own, place, send_sem, recv_sem):
        me = lax.axis_index('sp')
        self.me = me
        self.partner = me + 1 - 2 * lax.rem(me, 2)
        self.right = lax.rem(me + 2, seq_par)
        self.left = lax.rem(me + seq_par - 2, seq_par)
        self.far = lax.rem(me + 4, seq_par)
        self.other = lambda b: b + 1 - 2 * lax.rem(b, 2)
        both = slice(None)

        def remote(num, src, dst, to):
            return pltpu.make_async_remote_copy(src_ref=src, dst_ref=dst, send_sem=send_sem.at[num], recv_sem=recv_sem.at[num], device_id={'sp': to}, device_id_type=pl.DeviceIdType.MESH)

        self.r1 = remote(0, own(0), place(me, 0), self.right)
        self.l1 = remote(1, own(1), place(me, 1), self.left)
        self.r2 = remote(2, own(1), place(me, 1), self.right)
        self.l2 = remote(3, own(0), place(me, 0), self.left)
        self.p0 = remote(4, own(both), place(me, both), self.partner)
        self.r3 = remote(5, place(self.left, 0), place(self.left, 0), self.right)
        self.l3 = remote(6, place(self.right, 1), place(self.right, 1), self.left)
        self.p1 = remote(7, place(self.left, both), place(self.left, both), self.partner)
        self.p2 = remote(8, place(self.right, both), place(self.right, both), self.partner)
        self.p3 = remote(9, place(self.far, both), place(self.far, both), self.partner)

    def start(self):
        self.r1.start()
        self.l1.start()
        self.r2.start()
        self.l2.start()
        self.p0.start()

    def forward(self):
        self.r1.wait_recv()
        self.r3.start()
        self.l1.wait_recv()
        self.l3.start()

    def relay_near(self):
        self.r2.wait_recv()
        self.p1.start()
        self.l2.wait_recv()
        self.p2.start()

    def relay_far(self):
        self.r3.wait_recv()
        self.l3.wait_recv()
        self.p3.start()

    def finish_sends(self):
        for copy in (self.r1, self.l1, self.r2, self.l2, self.p0, self.r3, self.l3, self.p1, self.p2, self.p3):
            copy.wait_send()

    def finish_recvs(self):
        for copy in (self.p0, self.p1, self.p2, self.p3):
            copy.wait_recv()


GATHER_SEMS = [pltpu.SemaphoreType.DMA((10,)), pltpu.SemaphoreType.DMA((10,))]


def greet(seq_par):
    me = lax.axis_index('sp')
    barrier = pltpu.get_barrier_semaphore()
    for peer in (me + 1 - 2 * lax.rem(me, 2), lax.rem(me + 2, seq_par), lax.rem(me + seq_par - 2, seq_par)):
        pl.semaphore_signal(barrier, inc=1, device_id={'sp': peer}, device_id_type=pl.DeviceIdType.MESH)
    pl.semaphore_wait(barrier, 3)


def row_place(ref, rows):
    half = rows // 2

    def place(block, part):
        if isinstance(part, int):
            return ref.at[pl.ds(pl.multiple_of(block * rows + part * half, half), half), :]
        return ref.at[pl.ds(pl.multiple_of(block * rows, rows), rows), :]

    return place


def row_own(ref, rows):
    half = rows // 2

    def own(part):
        if isinstance(part, int):
            return ref.at[part * half:(part + 1) * half, :]
        return ref

    return own


class Bounce:
    def __init__(self, own, buffer, place, sems):
        self.fetch = pltpu.make_async_copy(own, buffer, sems.at[0])
        self.keep = pltpu.make_async_copy(buffer, place, sems.at[1])

    def turn(self):
        self.fetch.wait()
        self.keep.start()


def at_step(step):
    return pl.when(pl.program_id(0) == step)


def project_kernel(seq_par, group, own_ref, w_ref, cos_ref, sin_ref, all_ref, q_ref, k_ref, v_ref, tile, bounce, tile_sem, bounce_sem, send_sem, recv_sem):
    rows = own_ref.shape[0]
    dim = k_ref.shape[0]
    greet(seq_par)
    block_of = row_place(all_ref, rows)
    ring = RingGather(seq_par, row_own(own_ref, rows), block_of, send_sem, recv_sem)
    ring.start()

    def project(rows_ref, block):
        cols = pl.ds(pl.multiple_of(block * rows, rows), rows)
        cos_t = cos_ref[:, cols]
        sin_t = sin_ref[:, cols]
        lin = dot_nt(w_ref[...], rows_ref[...])
        for h in range(group + 2):
            part = lin[h * dim:(h + 1) * dim, :]
            if h < group:
                q_ref[h * dim:(h + 1) * dim, cols] = rotate(part, cos_t, sin_t).astype(BF16)
            elif h == group:
                k_ref[:, cols] = rotate(part, cos_t, sin_t).astype(BF16)
            else:
                v_ref[:, cols] = part.astype(BF16)

    def gathered(block):
        copy = pltpu.make_async_copy(block_of(block, slice(None)), tile, tile_sem)
        copy.start()
        copy.wait()
        project(tile, block)

    fetch = pltpu.make_async_copy(own_ref, bounce, bounce_sem)
    fetch.start()
    fetch.wait()
    keep = pltpu.make_async_copy(bounce, block_of(ring.me, slice(None)), bounce_sem)
    keep.start()
    project(bounce, ring.me)
    ring.p0.wait_recv()
    gathered(ring.partner)
    ring.forward()
    ring.relay_near()
    gathered(ring.left)
    gathered(ring.right)
    ring.p1.wait_recv()
    gathered(ring.other(ring.left))
    ring.p2.wait_recv()
    gathered(ring.other(ring.right))
    ring.relay_far()
    gathered(ring.far)
    ring.p3.wait_recv()
    gathered(ring.other(ring.far))
    keep.wait()
    ring.finish_sends()


def gather_project(normed, w_own, cos_t, sin_t, group, seq_par):
    rows, d_model = normed.shape
    dim = w_own.shape[0] // (group + 2)
    seq = rows * seq_par
    vmem = pl.BlockSpec(memory_space=pltpu.VMEM)
    hbm = pl.BlockSpec(memory_space=pl.ANY)
    return pl.pallas_call(
        functools.partial(project_kernel, seq_par, group),
        in_specs=[hbm, vmem, vmem, vmem],
        out_specs=[hbm, vmem, vmem, vmem],
        out_shape=[
            jax.ShapeDtypeStruct((seq, d_model), BF16),
            jax.ShapeDtypeStruct((group * dim, seq), BF16),
            jax.ShapeDtypeStruct((dim, seq), BF16),
            jax.ShapeDtypeStruct((dim, seq), BF16),
        ],
        scratch_shapes=[pltpu.VMEM((rows, d_model), BF16), pltpu.VMEM((rows, d_model), BF16), pltpu.SemaphoreType.DMA, pltpu.SemaphoreType.DMA] + GATHER_SEMS,
        compiler_params=pltpu.CompilerParams(collective_id=1, has_side_effects=True, vmem_limit_bytes=48 << 20),
        cost_estimate=pl.CostEstimate(flops=2 * seq * d_model * (group + 2) * dim, transcendentals=0, bytes_accessed=4 * seq * d_model),
        name='gather_project',
    )(normed, w_own, cos_t, sin_t)


def forward_kernel(seq_par, group, scale, q_ref, k_ref, v_ref, own_ref, o_ref, lse_ref, all_ref, bounce, bounce_sem, send_sem, recv_sem):
    block = pl.program_id(0)
    blocks = k_ref.shape[0] // BQ
    rows = own_ref.shape[0]
    place = row_place(all_ref, rows)
    ring = RingGather(seq_par, row_own(own_ref, rows), place, send_sem, recv_sem)
    local = Bounce(own_ref, bounce, place(ring.me, slice(None)), bounce_sem)

    @at_step(0)
    def _():
        greet(seq_par)
        ring.start()
        local.fetch.start()

    @at_step(1)
    def _():
        local.turn()

    @at_step(blocks * 7 // 12)
    def _():
        ring.forward()

    @at_step(blocks * 10 // 12)
    def _():
        ring.relay_near()

    dim = k_ref.shape[1]
    wide = group * BQ
    q_cat = heads_cat(q_ref, group)
    factor = scale * LOG2E

    def step(start, carry, masked):
        m_old, l_old, acc = carry
        keys = k_ref[pl.ds(start, BK), :]
        scores = dot(keys, q_cat) * factor
        if masked:
            row = lax.broadcasted_iota(jnp.int32, (BK, wide), 0)
            col = lax.broadcasted_iota(jnp.int32, (BK, wide), 1) % BQ
            scores = jnp.where(row <= col, scores, -1e30)
        m_new = jnp.maximum(m_old, jnp.max(scores, axis=0, keepdims=True))
        probs = jnp.exp2(scores - m_new)
        alpha = jnp.exp2(m_old - m_new)
        l_new = l_old * alpha + jnp.sum(probs, axis=0, keepdims=True)
        out = dot(v_ref[:, pl.ds(start, BK)], probs.astype(BF16))
        return m_new, l_new, acc * alpha + out

    init = (jnp.full((1, wide), -1e30, F32), jnp.zeros((1, wide), F32), jnp.zeros((dim, wide), F32))
    carry = lax.fori_loop(0, block, lambda i, c: step(pl.multiple_of(i * BK, BK), c, False), init)
    m_fin, l_fin, acc = step(pl.multiple_of(block * BK, BK), carry, True)
    out = (acc / l_fin).astype(BF16)
    lse = m_fin + jnp.log2(l_fin)
    for h in range(group):
        o_ref[h * dim:(h + 1) * dim, :] = out[:, h * BQ:(h + 1) * BQ]
        lse_ref[h:h + 1, :] = lse[:, h * BQ:(h + 1) * BQ]

    @at_step(blocks - 1)
    def _():
        ring.relay_far()
        local.keep.wait()
        ring.finish_recvs()
        ring.finish_sends()


def attention_forward(q_t, k_rows, v_t, d_out, group, seq_par):
    dim, seq = v_t.shape
    rows, d_model = d_out.shape
    scale = dim ** -0.5
    pairs = seq * (seq + BQ) // 2 * group
    hbm = pl.BlockSpec(memory_space=pl.ANY)
    return pl.pallas_call(
        functools.partial(forward_kernel, seq_par, group, scale),
        grid=(seq // BQ,),
        in_specs=[
            pl.BlockSpec((group * dim, BQ), lambda j: (0, j)),
            pl.BlockSpec((seq, dim), lambda j: (0, 0)),
            pl.BlockSpec((dim, seq), lambda j: (0, 0)),
            hbm,
        ],
        out_specs=[
            pl.BlockSpec((group * dim, BQ), lambda j: (0, j)),
            pl.BlockSpec((group, BQ), lambda j: (0, j)),
            hbm,
        ],
        out_shape=[
            jax.ShapeDtypeStruct((group * dim, seq), BF16),
            jax.ShapeDtypeStruct((group, seq), F32),
            jax.ShapeDtypeStruct((seq, d_model), BF16),
        ],
        scratch_shapes=[pltpu.VMEM((rows, d_model), BF16), pltpu.SemaphoreType.DMA((2,))] + GATHER_SEMS,
        compiler_params=pltpu.CompilerParams(collective_id=2, has_side_effects=True, vmem_limit_bytes=48 << 20),
        cost_estimate=pl.CostEstimate(flops=16 * pairs * dim, transcendentals=pairs, bytes_accessed=8 * group * dim * seq),
        name='attn_fwd',
    )(q_t, k_rows, v_t, d_out)


def backward_kernel(seq_par, group, scale, q_ref, dy_ref, wo_ref, o_ref, lse_ref, k_ref, v_ref, kt_ref, cos_ref, sin_ref, own_ref, dqb_ref, dk_ref, dv_ref, all_ref, dqa_ref, dk_acc, dv_acc, dq_buf, bounce, bounce_sem, send_sem, recv_sem, dqa_sem, dq_send, dq_recv):
    block = pl.program_id(0)
    blocks = k_ref.shape[0] // BQ
    dim = k_ref.shape[1]
    wide = group * BQ
    factor = scale * LOG2E
    rows = own_ref.shape[0]
    half = dqa_ref.shape[1]
    place = row_place(all_ref, rows)
    ring = RingGather(seq_par, row_own(own_ref, rows), place, send_sem, recv_sem)
    local = Bounce(own_ref, bounce, place(ring.me, slice(None)), bounce_sem)
    dq_place = row_place(dqa_ref, rows)
    dq_ring = RingGather(seq_par, lambda part: dq_place(ring.me, part), dq_place, dq_send, dq_recv)

    @at_step(0)
    def _():
        greet(seq_par)
        ring.start()
        local.fetch.start()
        dk_acc[...] = jnp.zeros_like(dk_acc)
        dv_acc[...] = jnp.zeros_like(dv_acc)

    @at_step(1)
    def _():
        local.turn()

    @at_step(blocks * 5 // 12)
    def _():
        ring.forward()

    @at_step(blocks * 8 // 12)
    def _():
        ring.relay_near()

    @at_step(blocks * 10 // 12)
    def _():
        ring.relay_far()
        store = pltpu.make_async_copy(dq_buf.at[:, :half], dq_place(ring.me, slice(None)), dqa_sem)
        store.start()
        store.wait()
        dq_ring.start()

    @at_step(blocks * 11 // 12)
    def _():
        dq_ring.forward()

    do_t = dot_nt(wo_ref[...], dy_ref[...]).astype(BF16)
    q_cat = heads_cat(q_ref, group)
    do_cat = jnp.concatenate([do_t[h * dim:(h + 1) * dim, :] for h in range(group)], axis=1)
    o_cat = heads_cat(o_ref, group)
    lse = jnp.concatenate([lse_ref[h:h + 1, :] for h in range(group)], axis=1)
    delta = jnp.sum(do_cat.astype(F32) * o_cat.astype(F32), axis=0, keepdims=True)

    def step(start, dq, masked):
        keys = pl.ds(start, BK)
        scores = dot(k_ref[keys, :], q_cat) * factor
        if masked:
            row = lax.broadcasted_iota(jnp.int32, (BK, wide), 0)
            col = lax.broadcasted_iota(jnp.int32, (BK, wide), 1) % BQ
            scores = jnp.where(row <= col, scores, -1e30)
        probs = jnp.exp2(scores - lse)
        d_probs = dot(v_ref[keys, :], do_cat).astype(BF16).astype(F32)
        d_scores = (probs * (d_probs - delta)).astype(BF16)
        dv_acc[:, keys] += dot_nt(do_cat, probs.astype(BF16))
        dk_acc[:, keys] += dot_nt(q_cat, d_scores)
        return dq + dot(kt_ref[:, keys], d_scores)

    dq = lax.fori_loop(0, block, lambda i, c: step(pl.multiple_of(i * BK, BK), c, False), jnp.zeros((dim, wide), F32))
    dq = step(pl.multiple_of(block * BK, BK), dq, True)
    dq = (dq * scale).astype(BF16).astype(F32)
    cols = pl.ds(pl.multiple_of(block * BQ, BQ), BQ)
    cos_t = cos_ref[:, cols]
    sin_t = sin_ref[:, cols]
    for h in range(group):
        dq_buf[h * dim:(h + 1) * dim, cols] = rotate_back(dq[:, h * BQ:(h + 1) * BQ], cos_t, sin_t).astype(BF16)

    @at_step(blocks - 1)
    def _():
        store = pltpu.make_async_copy(dq_buf.at[:, half:], dqb_ref, dqa_sem)
        store.start()
        dk = (dk_acc[...] * scale).astype(BF16).astype(F32)
        dk_ref[...] = rotate_back(dk, cos_ref[...], sin_ref[...]).astype(BF16)
        dv_ref[...] = dv_acc[...].astype(BF16)
        dq_ring.relay_near()
        ring.finish_recvs()
        ring.finish_sends()
        local.keep.wait()
        store.wait()
        dq_ring.relay_far()
        dq_ring.finish_recvs()
        dq_ring.finish_sends()


def attention_backward(q_t, dy_all, wo_own, o_t, lse, k_rows, v_rows, k_t, cos_t, sin_t, group, seq_par):
    dim, seq = k_t.shape
    rows, d_model = wo_own.shape
    scale = dim ** -0.5
    half = seq // 2
    pairs = seq * (seq + BQ) // 2 * group
    tile = pl.BlockSpec((rows, BQ), lambda j: (0, j))
    whole = lambda shape: pl.BlockSpec(shape, lambda j: (0, 0))
    hbm = pl.BlockSpec(memory_space=pl.ANY)
    return pl.pallas_call(
        functools.partial(backward_kernel, seq_par, group, scale),
        grid=(seq // BQ,),
        in_specs=[tile, pl.BlockSpec((BQ, d_model), lambda j: (j, 0)), whole(wo_own.shape), tile, pl.BlockSpec((group, BQ), lambda j: (0, j)), whole((seq, dim)), whole((seq, dim)), whole((dim, seq)), whole(cos_t.shape), whole(sin_t.shape), hbm],
        out_specs=[hbm, whole((dim, seq)), whole((dim, seq)), hbm, hbm],
        out_shape=[
            jax.ShapeDtypeStruct((rows, seq - half), BF16),
            jax.ShapeDtypeStruct((dim, seq), BF16),
            jax.ShapeDtypeStruct((dim, seq), BF16),
            jax.ShapeDtypeStruct((rows * seq_par, seq), BF16),
            jax.ShapeDtypeStruct((rows * seq_par, half), BF16),
        ],
        scratch_shapes=[pltpu.VMEM((dim, seq), F32), pltpu.VMEM((dim, seq), F32), pltpu.VMEM((rows, seq), BF16), pltpu.VMEM((rows, seq), BF16), pltpu.SemaphoreType.DMA((2,))] + GATHER_SEMS + [pltpu.SemaphoreType.DMA] + GATHER_SEMS,
        compiler_params=pltpu.CompilerParams(collective_id=3, has_side_effects=True, vmem_limit_bytes=56 << 20),
        cost_estimate=pl.CostEstimate(flops=40 * pairs * dim, transcendentals=pairs, bytes_accessed=12 * group * dim * seq),
        name='attn_bwd',
    )(q_t, dy_all, wo_own, o_t, lse, k_rows, v_rows, k_t, cos_t, sin_t, o_t)


def solution(mesh):
    seq_par = mesh.shape['sp']

    def local_step(x_local, dy_local, gain, w_q, w_k, w_v, w_o):
        _, seq_loc, d_model = x_local.shape
        num_q, dim = w_q.shape[1], w_q.shape[2]
        num_kv = w_k.shape[1]
        group = num_q // num_kv
        if num_kv != seq_par or seq_par % 4:
            raise ValueError('unsupported mesh')
        seq = seq_loc * seq_par
        index = lax.axis_index('sp')
        x_local = x_local[0]
        dy_local = dy_local[0]
        wq_t = jnp.transpose(w_q, (1, 2, 0)).reshape(num_q * dim, d_model)
        wk_t = jnp.transpose(w_k, (1, 2, 0)).reshape(num_kv * dim, d_model)
        wv_t = jnp.transpose(w_v, (1, 2, 0)).reshape(num_kv * dim, d_model)
        wo_t = w_o.reshape(num_q * dim, d_model)
        own_q = lambda w: lax.dynamic_slice_in_dim(w, index * group * dim, group * dim, 0)
        own_kv = lambda w: lax.dynamic_slice_in_dim(w, index * dim, dim, 0)
        gather = lambda a: lax.all_gather(a, 'sp', axis=0, tiled=True)

        cos_t, sin_t = rope_tables(jnp.arange(seq, dtype=F32), dim)
        x_hat, inv_rms, normed = norm_forward(x_local, gain)
        w_own = jnp.concatenate([own_q(wq_t), own_kv(wk_t), own_kv(wv_t)], axis=0)
        normed_all, q_t, k_t, v_t = gather_project(normed, w_own, cos_t, sin_t, group, seq_par)
        k_rows = k_t.T
        v_rows = v_t.T
        o_t, lse, dy_all = attention_forward(q_t, k_rows, v_t, dy_local, group, seq_par)
        dqb_t, dk_t, dv_t, o_all, dqa_all = attention_backward(q_t, dy_all, own_q(wo_t), o_t, lse, k_rows, v_rows, k_t, cos_t, sin_t, group, seq_par)
        dqb_all = gather(dqb_t)
        dk_all = gather(dk_t)
        dv_all = gather(dv_t)
        half = seq // 2
        at_col = lambda a, start: lax.dynamic_slice_in_dim(a, start, seq_loc, 1)
        mine = lambda a: at_col(a, index * seq_loc)
        back = lambda a, w: lax.dot_general(a, w, TN, preferred_element_type=F32)
        low = index * seq_loc < half
        dq_mine = jnp.where(low, at_col(dqa_all, jnp.where(low, index * seq_loc, 0)), at_col(dqb_all, jnp.where(low, 0, index * seq_loc - half)))
        y_out = (x_local.astype(F32) + back(mine(o_all), wo_t)).astype(BF16)
        d_wo = dot(o_all, dy_all)
        d_wqa = dot(dqa_all, normed_all[:half])
        d_wqa, dqb_all = lax.optimization_barrier((d_wqa, dqb_all))
        d_wq = d_wqa + dot(dqb_all, normed_all[half:])
        d_wk = dot(dk_all, normed_all)
        d_wv = dot(dv_all, normed_all)
        d_normed = (back(dq_mine, wq_t) + back(mine(dk_all), wk_t) + back(mine(dv_all), wv_t)).astype(BF16).astype(F32)
        d_gain = lax.psum(jnp.sum(d_normed * x_hat, axis=0), 'sp')
        d_hat = d_normed * gain
        d_x_norm = inv_rms * (d_hat - x_hat * jnp.mean(d_hat * x_hat, axis=-1, keepdims=True))
        d_x = (dy_local.astype(F32) + d_x_norm).astype(BF16)
        unflat = lambda g, heads: jnp.transpose(g.reshape(heads, dim, d_model), (2, 0, 1))
        return y_out[None], d_x[None], unflat(d_wq, num_q), unflat(d_wk, num_kv), unflat(d_wv, num_kv), d_wo.reshape(num_q, dim, d_model), d_gain

    specs_in = (P('dp', 'sp', None), P('dp', 'sp', None), P(None), P(None, None, None), P(None, None, None), P(None, None, None), P(None, None, None))
    specs_out = (P('dp', 'sp', None), P('dp', 'sp', None), P('dp', None, None), P('dp', None, None), P('dp', None, None), P('dp', None, None), P('dp'))
    return jax.shard_map(local_step, mesh=mesh, in_specs=specs_in, out_specs=specs_out, check_vma=False)
```

```python
import functools
import math
import jax
import jax.numpy as jnp
from jax import lax
from jax.experimental import pallas as pl
from jax.experimental.pallas import tpu as pltpu
from jax.sharding import PartitionSpec as P

ROPE_BASE = 1000000.0
NORM_EPS = 1e-5
LOG2E = math.log2(math.e)
BQ = 256
BK = 256
NT = (((1,), (1,)), ((), ()))
TN = (((0,), (0,)), ((), ()))
F32 = jnp.float32
BF16 = jnp.bfloat16


def rope_tables(positions, head_dim):
    half = head_dim // 2
    inv_freq = ROPE_BASE ** (-2.0 * jnp.arange(half, dtype=F32) / head_dim)
    angle = inv_freq[:, None] * positions[None, :]
    return jnp.cos(angle), jnp.sin(angle)


def rotate(vals, cos_t, sin_t):
    half = vals.shape[-2] // 2
    first = vals[..., :half, :]
    second = vals[..., half:, :]
    return jnp.concatenate([first * cos_t - second * sin_t, second * cos_t + first * sin_t], axis=-2)


def rotate_back(vals, cos_t, sin_t):
    half = vals.shape[-2] // 2
    first = vals[..., :half, :]
    second = vals[..., half:, :]
    return jnp.concatenate([first * cos_t + second * sin_t, second * cos_t - first * sin_t], axis=-2)


def norm_forward(x_local, gain):
    x_f32 = x_local.astype(F32)
    inv_rms = lax.rsqrt(jnp.mean(x_f32 * x_f32, axis=-1, keepdims=True) + NORM_EPS)
    return (x_f32 * inv_rms * gain).astype(BF16)


def dot(a, b):
    return jnp.dot(a, b, preferred_element_type=F32)


def dot_nt(a, b):
    return lax.dot_general(a, b, NT, preferred_element_type=F32)


def heads_cat(ref, num):
    dim = ref.shape[0] // num
    return jnp.concatenate([ref[h * dim:(h + 1) * dim, :] for h in range(num)], axis=1)


class RingGather:
    def __init__(self, seq_par, own, place, send_sem, recv_sem):
        me = lax.axis_index('sp')
        self.me = me
        self.partner = me + 1 - 2 * lax.rem(me, 2)
        self.right = lax.rem(me + 2, seq_par)
        self.left = lax.rem(me + seq_par - 2, seq_par)
        self.far = lax.rem(me + 4, seq_par)
        self.other = lambda b: b + 1 - 2 * lax.rem(b, 2)
        both = slice(None)

        def remote(num, src, dst, to):
            return pltpu.make_async_remote_copy(src_ref=src, dst_ref=dst, send_sem=send_sem.at[num], recv_sem=recv_sem.at[num], device_id={'sp': to}, device_id_type=pl.DeviceIdType.MESH)

        self.r1 = remote(0, own(0), place(me, 0), self.right)
        self.l1 = remote(1, own(1), place(me, 1), self.left)
        self.r2 = remote(2, own(1), place(me, 1), self.right)
        self.l2 = remote(3, own(0), place(me, 0), self.left)
        self.p0 = remote(4, own(both), place(me, both), self.partner)
        self.r3 = remote(5, place(self.left, 0), place(self.left, 0), self.right)
        self.l3 = remote(6, place(self.right, 1), place(self.right, 1), self.left)
        self.p1 = remote(7, place(self.left, both), place(self.left, both), self.partner)
        self.p2 = remote(8, place(self.right, both), place(self.right, both), self.partner)
        self.p3 = remote(9, place(self.far, both), place(self.far, both), self.partner)

    def start(self):
        self.r1.start()
        self.l1.start()
        self.r2.start()
        self.l2.start()
        self.p0.start()

    def forward(self):
        self.r1.wait_recv()
        self.r3.start()
        self.l1.wait_recv()
        self.l3.start()

    def relay_near(self):
        self.r2.wait_recv()
        self.p1.start()
        self.l2.wait_recv()
        self.p2.start()

    def relay_far(self):
        self.r3.wait_recv()
        self.l3.wait_recv()
        self.p3.start()

    def finish_sends(self):
        for copy in (self.r1, self.l1, self.r2, self.l2, self.p0, self.r3, self.l3, self.p1, self.p2, self.p3):
            copy.wait_send()

    def finish_recvs(self):
        for copy in (self.p0, self.p1, self.p2, self.p3):
            copy.wait_recv()


GATHER_SEMS = [pltpu.SemaphoreType.DMA((10,)), pltpu.SemaphoreType.DMA((10,))]


def greet(seq_par):
    me = lax.axis_index('sp')
    barrier = pltpu.get_barrier_semaphore()
    for peer in (me + 1 - 2 * lax.rem(me, 2), lax.rem(me + 2, seq_par), lax.rem(me + seq_par - 2, seq_par)):
        pl.semaphore_signal(barrier, inc=1, device_id={'sp': peer}, device_id_type=pl.DeviceIdType.MESH)
    pl.semaphore_wait(barrier, 3)


def row_place(ref, rows):
    half = rows // 2

    def place(block, part):
        if isinstance(part, int):
            return ref.at[pl.ds(pl.multiple_of(block * rows + part * half, half), half), :]
        return ref.at[pl.ds(pl.multiple_of(block * rows, rows), rows), :]

    return place


def row_own(ref, rows):
    half = rows // 2

    def own(part):
        if isinstance(part, int):
            return ref.at[part * half:(part + 1) * half, :]
        return ref

    return own


class Bounce:
    def __init__(self, own, buffer, place, sems):
        self.fetch = pltpu.make_async_copy(own, buffer, sems.at[0])
        self.keep = pltpu.make_async_copy(buffer, place, sems.at[1])

    def turn(self):
        self.fetch.wait()
        self.keep.start()


def at_step(step):
    return pl.when(pl.program_id(0) == step)


def project_kernel(seq_par, group, own_ref, wq_ref, wk_ref, wv_ref, cos_ref, sin_ref, all_ref, q_ref, k_ref, v_ref, k_rows_ref, v_rows_ref, tile, bounce, w_ref, tile_sem, bounce_sem, w_sem, send_sem, recv_sem):
    rows = own_ref.shape[0]
    dim = k_ref.shape[0]
    wide = group * dim
    me = lax.axis_index('sp')
    fetch = pltpu.make_async_copy(own_ref, bounce, bounce_sem)
    fetch.start()
    weights = [
        pltpu.make_async_copy(wq_ref.at[pl.ds(pl.multiple_of(me * wide, wide), wide), :], w_ref.at[:wide, :], w_sem.at[0]),
        pltpu.make_async_copy(wk_ref.at[pl.ds(pl.multiple_of(me * dim, dim), dim), :], w_ref.at[wide:wide + dim, :], w_sem.at[1]),
        pltpu.make_async_copy(wv_ref.at[pl.ds(pl.multiple_of(me * dim, dim), dim), :], w_ref.at[wide + dim:, :], w_sem.at[2]),
    ]
    for copy in weights:
        copy.start()
    greet(seq_par)
    block_of = row_place(all_ref, rows)
    ring = RingGather(seq_par, row_own(own_ref, rows), block_of, send_sem, recv_sem)
    ring.start()

    def project(rows_ref, block):
        cols = pl.ds(pl.multiple_of(block * rows, rows), rows)
        cos_t = cos_ref[:, cols]
        sin_t = sin_ref[:, cols]
        lin = dot_nt(w_ref[...], rows_ref[...])
        for h in range(group + 2):
            part = lin[h * dim:(h + 1) * dim, :]
            if h < group:
                q_ref[h * dim:(h + 1) * dim, cols] = rotate(part, cos_t, sin_t).astype(BF16)
            elif h == group:
                keys = rotate(part, cos_t, sin_t)
                k_ref[:, cols] = keys.astype(BF16)
                k_rows_ref[cols, :] = keys.T.astype(BF16)
            else:
                v_ref[:, cols] = part.astype(BF16)
                v_rows_ref[cols, :] = part.T.astype(BF16)

    def gathered(block):
        copy = pltpu.make_async_copy(block_of(block, slice(None)), tile, tile_sem)
        copy.start()
        copy.wait()
        project(tile, block)

    for copy in weights:
        copy.wait()
    fetch.wait()
    keep = pltpu.make_async_copy(bounce, block_of(ring.me, slice(None)), bounce_sem)
    keep.start()
    project(bounce, ring.me)
    ring.p0.wait_recv()
    gathered(ring.partner)
    ring.forward()
    ring.relay_near()
    gathered(ring.left)
    gathered(ring.right)
    ring.p1.wait_recv()
    gathered(ring.other(ring.left))
    ring.p2.wait_recv()
    gathered(ring.other(ring.right))
    ring.relay_far()
    gathered(ring.far)
    ring.p3.wait_recv()
    gathered(ring.other(ring.far))
    keep.wait()
    ring.finish_sends()


def gather_project(normed, wq_t, wk_t, wv_t, cos_t, sin_t, group, seq_par):
    rows, d_model = normed.shape
    dim = 2 * cos_t.shape[0]
    seq = rows * seq_par
    vmem = pl.BlockSpec(memory_space=pltpu.VMEM)
    hbm = pl.BlockSpec(memory_space=pl.ANY)
    return pl.pallas_call(
        functools.partial(project_kernel, seq_par, group),
        in_specs=[hbm, hbm, hbm, hbm, vmem, vmem],
        out_specs=[hbm, vmem, vmem, vmem, vmem, vmem],
        out_shape=[
            jax.ShapeDtypeStruct((seq, d_model), BF16),
            jax.ShapeDtypeStruct((group * dim, seq), BF16),
            jax.ShapeDtypeStruct((dim, seq), BF16),
            jax.ShapeDtypeStruct((dim, seq), BF16),
            jax.ShapeDtypeStruct((seq, dim), BF16),
            jax.ShapeDtypeStruct((seq, dim), BF16),
        ],
        scratch_shapes=[pltpu.VMEM((rows, d_model), BF16), pltpu.VMEM((rows, d_model), BF16), pltpu.VMEM(((group + 2) * dim, d_model), BF16), pltpu.SemaphoreType.DMA, pltpu.SemaphoreType.DMA, pltpu.SemaphoreType.DMA((3,))] + GATHER_SEMS,
        compiler_params=pltpu.CompilerParams(collective_id=1, has_side_effects=True, vmem_limit_bytes=48 << 20),
        cost_estimate=pl.CostEstimate(flops=2 * seq * d_model * (group + 2) * dim, transcendentals=0, bytes_accessed=4 * seq * d_model),
        name='gather_project',
    )(normed, wq_t, wk_t, wv_t, cos_t, sin_t)


def forward_kernel(seq_par, group, scale, q_ref, k_ref, v_ref, own_ref, o_ref, lse_ref, all_ref, bounce, bounce_sem, send_sem, recv_sem):
    block = pl.program_id(0)
    blocks = k_ref.shape[0] // BQ
    rows = own_ref.shape[0]
    place = row_place(all_ref, rows)
    ring = RingGather(seq_par, row_own(own_ref, rows), place, send_sem, recv_sem)
    local = Bounce(own_ref, bounce, place(ring.me, slice(None)), bounce_sem)

    @at_step(0)
    def _():
        greet(seq_par)
        ring.start()
        local.fetch.start()

    @at_step(1)
    def _():
        local.turn()

    @at_step(blocks * 7 // 12)
    def _():
        ring.forward()

    @at_step(blocks * 10 // 12)
    def _():
        ring.relay_near()

    dim = k_ref.shape[1]
    wide = group * BQ
    q_cat = heads_cat(q_ref, group)
    factor = scale * LOG2E

    def step(start, carry, masked):
        m_old, l_old, acc = carry
        keys = k_ref[pl.ds(start, BK), :]
        scores = dot(keys, q_cat) * factor
        if masked:
            row = lax.broadcasted_iota(jnp.int32, (BK, wide), 0)
            col = lax.broadcasted_iota(jnp.int32, (BK, wide), 1) % BQ
            scores = jnp.where(row <= col, scores, -1e30)
        m_new = jnp.maximum(m_old, jnp.max(scores, axis=0, keepdims=True))
        probs = jnp.exp2(scores - m_new)
        alpha = jnp.exp2(m_old - m_new)
        l_new = l_old * alpha + jnp.sum(probs, axis=0, keepdims=True)
        out = dot(v_ref[:, pl.ds(start, BK)], probs.astype(BF16))
        return m_new, l_new, acc * alpha + out

    init = (jnp.full((1, wide), -1e30, F32), jnp.zeros((1, wide), F32), jnp.zeros((dim, wide), F32))
    carry = lax.fori_loop(0, block, lambda i, c: step(pl.multiple_of(i * BK, BK), c, False), init)
    m_fin, l_fin, acc = step(pl.multiple_of(block * BK, BK), carry, True)
    out = (acc / l_fin).astype(BF16)
    lse = m_fin + jnp.log2(l_fin)
    for h in range(group):
        o_ref[h * dim:(h + 1) * dim, :] = out[:, h * BQ:(h + 1) * BQ]
        lse_ref[h:h + 1, :] = lse[:, h * BQ:(h + 1) * BQ]

    @at_step(blocks - 1)
    def _():
        ring.relay_far()
        local.keep.wait()
        ring.finish_recvs()
        ring.finish_sends()


def attention_forward(q_t, k_rows, v_t, d_out, group, seq_par):
    dim, seq = v_t.shape
    rows, d_model = d_out.shape
    scale = dim ** -0.5
    pairs = seq * (seq + BQ) // 2 * group
    hbm = pl.BlockSpec(memory_space=pl.ANY)
    return pl.pallas_call(
        functools.partial(forward_kernel, seq_par, group, scale),
        grid=(seq // BQ,),
        in_specs=[
            pl.BlockSpec((group * dim, BQ), lambda j: (0, j)),
            pl.BlockSpec((seq, dim), lambda j: (0, 0)),
            pl.BlockSpec((dim, seq), lambda j: (0, 0)),
            hbm,
        ],
        out_specs=[
            pl.BlockSpec((group * dim, BQ), lambda j: (0, j)),
            pl.BlockSpec((group, BQ), lambda j: (0, j)),
            hbm,
        ],
        out_shape=[
            jax.ShapeDtypeStruct((group * dim, seq), BF16),
            jax.ShapeDtypeStruct((group, seq), F32),
            jax.ShapeDtypeStruct((seq, d_model), BF16),
        ],
        scratch_shapes=[pltpu.VMEM((rows, d_model), BF16), pltpu.SemaphoreType.DMA((2,))] + GATHER_SEMS,
        compiler_params=pltpu.CompilerParams(collective_id=2, has_side_effects=True, vmem_limit_bytes=48 << 20),
        cost_estimate=pl.CostEstimate(flops=16 * pairs * dim, transcendentals=pairs, bytes_accessed=8 * group * dim * seq),
        name='attn_fwd',
    )(q_t, k_rows, v_t, d_out)


def backward_kernel(seq_par, group, scale, q_ref, dy_ref, wo_ref, o_ref, lse_ref, k_ref, v_ref, kt_ref, cos_ref, sin_ref, own_ref, x_ref, dqb_ref, dkv_ref, y_ref, all_ref, dqa_ref, dk_acc, dv_acc, dq_buf, bounce, wo_buf, wo_sem, o_mine, o_rows, o_sem, bounce_sem, send_sem, recv_sem, dqa_sem, dq_send, dq_recv):
    block = pl.program_id(0)
    blocks = k_ref.shape[0] // BQ
    dim = k_ref.shape[1]
    wide = group * BQ
    factor = scale * LOG2E
    rows = own_ref.shape[0]
    half = dqa_ref.shape[1]
    place = row_place(all_ref, rows)
    ring = RingGather(seq_par, row_own(own_ref, rows), place, send_sem, recv_sem)
    local = Bounce(own_ref, bounce, place(ring.me, slice(None)), bounce_sem)
    dq_place = row_place(dqa_ref, rows)
    dq_ring = RingGather(seq_par, lambda part: dq_place(ring.me, part), dq_place, dq_send, dq_recv)

    @at_step(0)
    def _():
        weights = pltpu.make_async_copy(wo_ref, wo_buf, wo_sem)
        weights.start()
        greet(seq_par)
        ring.start()
        local.fetch.start()
        weights.wait()
        dk_acc[...] = jnp.zeros_like(dk_acc)
        dv_acc[...] = jnp.zeros_like(dv_acc)

    @at_step(1)
    def _():
        local.turn()

    @at_step(blocks * 5 // 12)
    def _():
        ring.forward()

    @at_step(blocks * 8 // 12)
    def _():
        ring.relay_near()
        store = pltpu.make_async_copy(dq_buf.at[:, :half], dq_place(ring.me, slice(None)), dqa_sem)
        store.start()
        store.wait()
        dq_ring.start()

    @at_step(blocks * 10 // 12)
    def _():
        ring.relay_far()

    @at_step(blocks * 11 // 12)
    def _():
        dq_ring.forward()

    do_t = dot_nt(wo_buf[pl.ds(pl.multiple_of(ring.me * rows, rows), rows), :], dy_ref[...]).astype(BF16)
    q_cat = heads_cat(q_ref, group)
    do_cat = jnp.concatenate([do_t[h * dim:(h + 1) * dim, :] for h in range(group)], axis=1)
    o_cat = heads_cat(o_ref, group)
    lse = jnp.concatenate([lse_ref[h:h + 1, :] for h in range(group)], axis=1)
    delta = jnp.sum(do_cat.astype(F32) * o_cat.astype(F32), axis=0, keepdims=True)

    def step(start, dq, masked):
        keys = pl.ds(start, BK)
        scores = dot(k_ref[keys, :], q_cat) * factor
        if masked:
            row = lax.broadcasted_iota(jnp.int32, (BK, wide), 0)
            col = lax.broadcasted_iota(jnp.int32, (BK, wide), 1) % BQ
            scores = jnp.where(row <= col, scores, -1e30)
        probs = jnp.exp2(scores - lse)
        d_probs = dot(v_ref[keys, :], do_cat).astype(BF16).astype(F32)
        d_scores = (probs * (d_probs - delta)).astype(BF16)
        dv_acc[:, keys] += dot_nt(do_cat, probs.astype(BF16))
        dk_acc[:, keys] += dot_nt(q_cat, d_scores)
        return dq + dot(kt_ref[:, keys], d_scores)

    dq = lax.fori_loop(0, block, lambda i, c: step(pl.multiple_of(i * BK, BK), c, False), jnp.zeros((dim, wide), F32))
    dq = step(pl.multiple_of(block * BK, BK), dq, True)
    dq = (dq * scale).astype(BF16).astype(F32)
    cols = pl.ds(pl.multiple_of(block * BQ, BQ), BQ)
    cos_t = cos_ref[:, cols]
    sin_t = sin_ref[:, cols]
    for h in range(group):
        dq_buf[h * dim:(h + 1) * dim, cols] = rotate_back(dq[:, h * BQ:(h + 1) * BQ], cos_t, sin_t).astype(BF16)

    @at_step(blocks - 1)
    def _():
        store = pltpu.make_async_copy(dq_buf.at[:, half:], dqb_ref, dqa_sem)
        store.start()
        dk = (dk_acc[...] * scale).astype(BF16).astype(F32)
        dkv_ref[:dim, :] = rotate_back(dk, cos_ref[...], sin_ref[...]).astype(BF16)
        dkv_ref[dim:, :] = dv_acc[...].astype(BF16)
        dq_ring.relay_near()
        ring.finish_recvs()
        ring.finish_sends()
        local.keep.wait()
        store.wait()
        tokens = x_ref.shape[0]
        fetch = pltpu.make_async_copy(all_ref.at[:, pl.ds(pl.multiple_of(ring.me * tokens, tokens), tokens)], o_mine, o_sem)
        fetch.start()
        fetch.wait()
        o_rows[...] = o_mine[...].T
        d_model = x_ref.shape[1]
        wide_y = math.gcd(d_model, 512)
        for start_y in range(0, d_model, wide_y):
            cols_y = slice(start_y, start_y + wide_y)
            y_ref[:, cols_y] = (x_ref[:, cols_y].astype(F32) + dot(o_rows[...], wo_buf[:, cols_y])).astype(BF16)
        dq_ring.relay_far()
        dq_ring.finish_recvs()
        dq_ring.finish_sends()


def attention_backward(x_local, q_t, dy_all, wo_t, o_t, lse, k_rows, v_rows, k_t, cos_t, sin_t, group, seq_par):
    dim, seq = k_t.shape
    rows, d_model = q_t.shape[0], wo_t.shape[1]
    scale = dim ** -0.5
    half = seq // 2
    pairs = seq * (seq + BQ) // 2 * group
    tile = pl.BlockSpec((rows, BQ), lambda j: (0, j))
    whole = lambda shape: pl.BlockSpec(shape, lambda j: (0, 0))
    hbm = pl.BlockSpec(memory_space=pl.ANY)
    return pl.pallas_call(
        functools.partial(backward_kernel, seq_par, group, scale),
        grid=(seq // BQ,),
        in_specs=[tile, pl.BlockSpec((BQ, d_model), lambda j: (j, 0)), hbm, tile, pl.BlockSpec((group, BQ), lambda j: (0, j)), whole((seq, dim)), whole((seq, dim)), whole((dim, seq)), whole(cos_t.shape), whole(sin_t.shape), hbm, whole(x_local.shape)],
        out_specs=[hbm, whole((2 * dim, seq)), whole(x_local.shape), hbm, hbm],
        out_shape=[
            jax.ShapeDtypeStruct((rows, seq - half), BF16),
            jax.ShapeDtypeStruct((2 * dim, seq), BF16),
            jax.ShapeDtypeStruct(x_local.shape, BF16),
            jax.ShapeDtypeStruct((rows * seq_par, seq), BF16),
            jax.ShapeDtypeStruct((rows * seq_par, half), BF16),
        ],
        scratch_shapes=[pltpu.VMEM((dim, seq), F32), pltpu.VMEM((dim, seq), F32), pltpu.VMEM((rows, seq), BF16), pltpu.VMEM((rows, seq), BF16), pltpu.VMEM(wo_t.shape, BF16), pltpu.SemaphoreType.DMA, pltpu.VMEM((wo_t.shape[0], x_local.shape[0]), BF16), pltpu.VMEM((x_local.shape[0], wo_t.shape[0]), BF16), pltpu.SemaphoreType.DMA, pltpu.SemaphoreType.DMA((2,))] + GATHER_SEMS + [pltpu.SemaphoreType.DMA] + GATHER_SEMS,
        compiler_params=pltpu.CompilerParams(collective_id=3, has_side_effects=True, vmem_limit_bytes=56 << 20),
        cost_estimate=pl.CostEstimate(flops=40 * pairs * dim, transcendentals=pairs, bytes_accessed=12 * group * dim * seq),
        name='attn_bwd',
    )(q_t, dy_all, wo_t, o_t, lse, k_rows, v_rows, k_t, cos_t, sin_t, o_t, x_local)


def outer_kernel(*refs):
    *parts, rhs_ref, out_ref = refs
    start = 0
    total = None
    for part in parts:
        depth = part.shape[1]
        term = dot(part[...], rhs_ref[start:start + depth, :])
        total = term if total is None else total + term
        start += depth
    out_ref[...] = total


def weight_grad(parts, rhs, name):
    rows = parts[0].shape[0]
    depth, d_model = rhs.shape
    tall = math.gcd(rows, 256)
    return pl.pallas_call(
        outer_kernel,
        grid=(rows // tall,),
        in_specs=[pl.BlockSpec((tall, p.shape[1]), lambda m: (m, 0)) for p in parts] + [pl.BlockSpec((depth, d_model), lambda m: (0, 0))],
        out_specs=pl.BlockSpec((tall, d_model), lambda m: (m, 0)),
        out_shape=jax.ShapeDtypeStruct((rows, d_model), F32),
        compiler_params=pltpu.CompilerParams(vmem_limit_bytes=60 << 20),
        cost_estimate=pl.CostEstimate(flops=2 * rows * depth * d_model, transcendentals=0, bytes_accessed=2 * depth * (rows + d_model) + 4 * rows * d_model),
        name=name,
    )(*parts, rhs)


def pair_kernel(dim, lhs_ref, rhs_ref, dk_ref, dv_ref):
    both = dot(lhs_ref[...], rhs_ref[...])
    for h in range(dk_ref.shape[0] // dim):
        dk_ref[h * dim:(h + 1) * dim, :] = both[2 * h * dim:(2 * h + 1) * dim, :]
        dv_ref[h * dim:(h + 1) * dim, :] = both[(2 * h + 1) * dim:(2 * h + 2) * dim, :]


def pair_grad(lhs, rhs, dim):
    rows, depth = lhs.shape
    d_model = rhs.shape[1]
    tall = math.gcd(rows, 256)
    out = pl.BlockSpec((tall // 2, d_model), lambda m: (m, 0))
    return pl.pallas_call(
        functools.partial(pair_kernel, dim),
        grid=(rows // tall,),
        in_specs=[pl.BlockSpec((tall, depth), lambda m: (m, 0)), pl.BlockSpec((depth, d_model), lambda m: (0, 0))],
        out_specs=[out, out],
        out_shape=[jax.ShapeDtypeStruct((rows // 2, d_model), F32)] * 2,
        compiler_params=pltpu.CompilerParams(vmem_limit_bytes=60 << 20),
        cost_estimate=pl.CostEstimate(flops=2 * rows * depth * d_model, transcendentals=0, bytes_accessed=2 * depth * (rows + d_model) + 4 * rows * d_model),
        name='d_wkv',
    )(lhs, rhs)


def input_grad_kernel(seq_par, dqa_ref, dqb_ref, dkv_ref, wq_ref, wk_ref, wv_ref, x_ref, dy_ref, gain_ref, dx_ref, dgain_ref, dq_buf, dk_buf, dv_buf, wq_buf, wk_buf, wv_buf, acc, part, slots, act_sem, w_sem, send_sem, recv_sem):
    me = lax.axis_index('sp')
    tokens, d_model = x_ref.shape
    half = dqa_ref.shape[1]
    barrier = pltpu.get_barrier_semaphore()
    for step in range(1, seq_par):
        pl.semaphore_signal(barrier, inc=1, device_id={'sp': lax.rem(me + step, seq_par)}, device_id_type=pl.DeviceIdType.MESH)
    low = me * tokens < half
    first = pl.multiple_of(jnp.where(low, me * tokens, 0), 128)
    second = pl.multiple_of(jnp.where(low, 0, me * tokens - half), 128)
    cols = pl.ds(pl.multiple_of(me * tokens, tokens), tokens)
    from_a = pltpu.make_async_copy(dqa_ref.at[:, pl.ds(first, tokens)], dq_buf, act_sem.at[0])
    from_b = pltpu.make_async_copy(dqb_ref.at[:, pl.ds(second, tokens)], dq_buf, act_sem.at[0])

    @pl.when(low)
    def _():
        from_a.start()

    @pl.when(jnp.logical_not(low))
    def _():
        from_b.start()

    take_k = pltpu.make_async_copy(dkv_ref.at[:, 0, :, cols], dk_buf, act_sem.at[1])
    take_v = pltpu.make_async_copy(dkv_ref.at[:, 1, :, cols], dv_buf, act_sem.at[2])
    take_k.start()
    take_v.start()
    chunk = wq_buf.shape[0] // 4
    loads = [pltpu.make_async_copy(wq_ref.at[c * chunk:(c + 1) * chunk, :], wq_buf.at[c * chunk:(c + 1) * chunk, :], w_sem.at[c]) for c in range(4)]
    loads += [pltpu.make_async_copy(wk_ref, wk_buf, w_sem.at[4]), pltpu.make_async_copy(wv_ref, wv_buf, w_sem.at[5])]
    for copy in loads:
        copy.start()
    from_a.wait()
    for c in range(4):
        loads[c].wait()
        term = dot(dq_buf[c * chunk:(c + 1) * chunk, :].T, wq_buf[c * chunk:(c + 1) * chunk, :])
        if c == 0:
            acc[...] = term
        else:
            acc[...] += term
    take_k.wait()
    take_v.wait()
    loads[4].wait()
    loads[5].wait()
    acc[...] += dot(dk_buf[...].reshape(wk_buf.shape[0], tokens).T, wk_buf[...])
    acc[...] += dot(dv_buf[...].reshape(wv_buf.shape[0], tokens).T, wv_buf[...])
    d_normed = acc[...].astype(BF16).astype(F32)
    acc[...] = d_normed
    x_f32 = x_ref[...].astype(F32)
    inv_rms = lax.rsqrt(jnp.mean(x_f32 * x_f32, axis=-1, keepdims=True) + NORM_EPS)
    part[...] = jnp.sum(d_normed * (x_f32 * inv_rms), axis=0, keepdims=True)
    dots = jnp.mean(acc[...] * gain_ref[...] * (x_ref[...].astype(F32) * inv_rms), axis=-1, keepdims=True)
    x_hat = x_ref[...].astype(F32) * inv_rms
    dx_ref[...] = (dy_ref[...].astype(F32) + inv_rms * (acc[...] * gain_ref[...] - x_hat * dots)).astype(BF16)
    pl.semaphore_wait(barrier, seq_par - 1)
    copies = []
    for step in range(1, seq_par):
        copies.append(pltpu.make_async_remote_copy(src_ref=part, dst_ref=slots.at[me], send_sem=send_sem.at[step], recv_sem=recv_sem.at[step], device_id={'sp': lax.rem(me + step, seq_par)}, device_id_type=pl.DeviceIdType.MESH))
        copies[-1].start()
    slots[me] = part[...]
    for copy in copies:
        copy.wait_recv()
    total = slots[0]
    for step in range(1, seq_par):
        total = total + slots[step]
    dgain_ref[...] = total
    for copy in copies:
        copy.wait_send()


def input_grad(dqa_all, dqb_all, dkv_all, wq_t, wk_t, wv_t, x_local, dy_local, gain, dim, seq_par):
    tokens, d_model = x_local.shape
    num_kv = wk_t.shape[0] // dim
    seq = dkv_all.shape[1]
    vmem = pl.BlockSpec(memory_space=pltpu.VMEM)
    hbm = pl.BlockSpec(memory_space=pl.ANY)
    return pl.pallas_call(
        functools.partial(input_grad_kernel, seq_par),
        in_specs=[hbm] * 6 + [vmem] * 3,
        out_specs=[vmem, vmem],
        out_shape=[jax.ShapeDtypeStruct(x_local.shape, BF16), jax.ShapeDtypeStruct((1, d_model), F32)],
        scratch_shapes=[
            pltpu.VMEM((wq_t.shape[0], tokens), BF16),
            pltpu.VMEM((num_kv, dim, tokens), BF16),
            pltpu.VMEM((num_kv, dim, tokens), BF16),
            pltpu.VMEM(wq_t.shape, BF16),
            pltpu.VMEM(wk_t.shape, BF16),
            pltpu.VMEM(wv_t.shape, BF16),
            pltpu.VMEM((tokens, d_model), F32),
            pltpu.VMEM((1, d_model), F32),
            pltpu.VMEM((seq_par, 1, d_model), F32),
            pltpu.SemaphoreType.DMA((3,)),
            pltpu.SemaphoreType.DMA((6,)),
            pltpu.SemaphoreType.DMA((seq_par,)),
            pltpu.SemaphoreType.DMA((seq_par,)),
        ],
        compiler_params=pltpu.CompilerParams(collective_id=4, has_side_effects=True, vmem_limit_bytes=56 << 20),
        cost_estimate=pl.CostEstimate(flops=2 * tokens * d_model * (wq_t.shape[0] + 2 * wk_t.shape[0]), transcendentals=0, bytes_accessed=2 * d_model * (wq_t.shape[0] + 2 * wk_t.shape[0])),
        name='input_grad',
    )(dqa_all, dqb_all, dkv_all.reshape(num_kv, 2, dim, seq), wq_t, wk_t, wv_t, x_local, dy_local, gain[None])


def solution(mesh):
    seq_par = mesh.shape['sp']

    def local_step(x_local, dy_local, gain, w_q, w_k, w_v, w_o):
        _, seq_loc, d_model = x_local.shape
        num_q, dim = w_q.shape[1], w_q.shape[2]
        num_kv = w_k.shape[1]
        group = num_q // num_kv
        if num_kv != seq_par or seq_par % 4:
            raise ValueError('unsupported mesh')
        seq = seq_loc * seq_par
        x_local = x_local[0]
        dy_local = dy_local[0]
        wq_t = jnp.transpose(w_q, (1, 2, 0)).reshape(num_q * dim, d_model)
        wk_t = jnp.transpose(w_k, (1, 2, 0)).reshape(num_kv * dim, d_model)
        wv_t = jnp.transpose(w_v, (1, 2, 0)).reshape(num_kv * dim, d_model)
        wo_t = w_o.reshape(num_q * dim, d_model)
        gather = lambda a: lax.all_gather(a, 'sp', axis=0, tiled=True)

        cos_t, sin_t = rope_tables(jnp.arange(seq, dtype=F32), dim)
        normed = norm_forward(x_local, gain)
        normed_all, q_t, k_t, v_t, k_rows, v_rows = gather_project(normed, wq_t, wk_t, wv_t, cos_t, sin_t, group, seq_par)
        o_t, lse, dy_all = attention_forward(q_t, k_rows, v_t, dy_local, group, seq_par)
        dqb_t, dkv_t, y_out, o_all, dqa_all = attention_backward(x_local, q_t, dy_all, wo_t, o_t, lse, k_rows, v_rows, k_t, cos_t, sin_t, group, seq_par)
        dqb_all = gather(dqb_t)
        d_wo = weight_grad([o_all], dy_all, 'd_wo')
        dkv_t, d_wo = lax.optimization_barrier((dkv_t, d_wo))
        dkv_all = gather(dkv_t)
        d_wq = weight_grad([dqa_all, dqb_all], normed_all, 'd_wq')
        dkv_all, d_wq = lax.optimization_barrier((dkv_all, d_wq))
        d_wk, d_wv = pair_grad(dkv_all, normed_all, dim)
        d_x, d_gain = input_grad(dqa_all, dqb_all, dkv_all, wq_t, wk_t, wv_t, x_local, dy_local, gain, dim, seq_par)
        unflat = lambda g, heads: jnp.transpose(g.reshape(heads, dim, d_model), (2, 0, 1))
        return y_out[None], d_x[None], unflat(d_wq, num_q), unflat(d_wk, num_kv), unflat(d_wv, num_kv), d_wo.reshape(num_q, dim, d_model), d_gain[0]

    specs_in = (P('dp', 'sp', None), P('dp', 'sp', None), P(None), P(None, None, None), P(None, None, None), P(None, None, None), P(None, None, None))
    specs_out = (P('dp', 'sp', None), P('dp', 'sp', None), P('dp', None, None), P('dp', None, None), P('dp', None, None), P('dp', None, None), P('dp'))
    return jax.shard_map(local_step, mesh=mesh, in_specs=specs_in, out_specs=specs_out, check_vma=False)
```

```python
import functools
import math
import jax
import jax.numpy as jnp
from jax import lax
from jax.experimental import pallas as pl
from jax.experimental.pallas import tpu as pltpu
from jax.sharding import PartitionSpec as P

ROPE_BASE = 1000000.0
NORM_EPS = 1e-5
LOG2E = math.log2(math.e)
BQ = 256
BK = 256
NT = (((1,), (1,)), ((), ()))
TN = (((0,), (0,)), ((), ()))
F32 = jnp.float32
BF16 = jnp.bfloat16


def rope_tables(positions, head_dim):
    half = head_dim // 2
    inv_freq = ROPE_BASE ** (-2.0 * jnp.arange(half, dtype=F32) / head_dim)
    angle = inv_freq[:, None] * positions[None, :]
    return jnp.cos(angle), jnp.sin(angle)


def rotate(vals, cos_t, sin_t):
    half = vals.shape[-2] // 2
    first = vals[..., :half, :]
    second = vals[..., half:, :]
    return jnp.concatenate([first * cos_t - second * sin_t, second * cos_t + first * sin_t], axis=-2)


def rotate_back(vals, cos_t, sin_t):
    half = vals.shape[-2] // 2
    first = vals[..., :half, :]
    second = vals[..., half:, :]
    return jnp.concatenate([first * cos_t + second * sin_t, second * cos_t - first * sin_t], axis=-2)


def norm_forward(x_local, gain):
    x_f32 = x_local.astype(F32)
    inv_rms = lax.rsqrt(jnp.mean(x_f32 * x_f32, axis=-1, keepdims=True) + NORM_EPS)
    return (x_f32 * inv_rms * gain).astype(BF16)


def dot(a, b):
    return jnp.dot(a, b, preferred_element_type=F32)


def dot_nt(a, b):
    return lax.dot_general(a, b, NT, preferred_element_type=F32)


def heads_cat(ref, num):
    dim = ref.shape[0] // num
    return jnp.concatenate([ref[h * dim:(h + 1) * dim, :] for h in range(num)], axis=1)


class RingGather:
    def __init__(self, seq_par, own, place, send_sem, recv_sem):
        me = lax.axis_index('sp')
        self.me = me
        self.partner = me + 1 - 2 * lax.rem(me, 2)
        self.right = lax.rem(me + 2, seq_par)
        self.left = lax.rem(me + seq_par - 2, seq_par)
        self.far = lax.rem(me + 4, seq_par)
        self.other = lambda b: b + 1 - 2 * lax.rem(b, 2)
        both = slice(None)

        def remote(num, src, dst, to):
            return pltpu.make_async_remote_copy(src_ref=src, dst_ref=dst, send_sem=send_sem.at[num], recv_sem=recv_sem.at[num], device_id={'sp': to}, device_id_type=pl.DeviceIdType.MESH)

        self.r1 = remote(0, own(0), place(me, 0), self.right)
        self.l1 = remote(1, own(1), place(me, 1), self.left)
        self.r2 = remote(2, own(1), place(me, 1), self.right)
        self.l2 = remote(3, own(0), place(me, 0), self.left)
        self.p0 = remote(4, own(both), place(me, both), self.partner)
        self.r3 = remote(5, place(self.left, 0), place(self.left, 0), self.right)
        self.l3 = remote(6, place(self.right, 1), place(self.right, 1), self.left)
        self.p1 = remote(7, place(self.left, both), place(self.left, both), self.partner)
        self.p2 = remote(8, place(self.right, both), place(self.right, both), self.partner)
        self.p3 = remote(9, place(self.far, both), place(self.far, both), self.partner)

    def start(self):
        self.r1.start()
        self.l1.start()
        self.r2.start()
        self.l2.start()
        self.p0.start()

    def forward(self):
        self.r1.wait_recv()
        self.r3.start()
        self.l1.wait_recv()
        self.l3.start()

    def relay_near(self):
        self.r2.wait_recv()
        self.p1.start()
        self.l2.wait_recv()
        self.p2.start()

    def relay_far(self):
        self.r3.wait_recv()
        self.l3.wait_recv()
        self.p3.start()

    def finish_sends(self):
        for copy in (self.r1, self.l1, self.r2, self.l2, self.p0, self.r3, self.l3, self.p1, self.p2, self.p3):
            copy.wait_send()

    def finish_recvs(self):
        for copy in (self.p0, self.p1, self.p2, self.p3):
            copy.wait_recv()


GATHER_SEMS = [pltpu.SemaphoreType.DMA((10,)), pltpu.SemaphoreType.DMA((10,))]


def greet(seq_par, meanwhile=None):
    me = lax.axis_index('sp')
    barrier = pltpu.get_barrier_semaphore()
    for peer in (me + 1 - 2 * lax.rem(me, 2), lax.rem(me + 2, seq_par), lax.rem(me + seq_par - 2, seq_par)):
        pl.semaphore_signal(barrier, inc=1, device_id={'sp': peer}, device_id_type=pl.DeviceIdType.MESH)
    if meanwhile is not None:
        meanwhile()
    pl.semaphore_wait(barrier, 3)


def row_place(ref, rows):
    half = rows // 2

    def place(block, part):
        if isinstance(part, int):
            return ref.at[pl.ds(pl.multiple_of(block * rows + part * half, half), half), :]
        return ref.at[pl.ds(pl.multiple_of(block * rows, rows), rows), :]

    return place


def row_own(ref, rows):
    half = rows // 2

    def own(part):
        if isinstance(part, int):
            return ref.at[part * half:(part + 1) * half, :]
        return ref

    return own


class Bounce:
    def __init__(self, own, buffer, place, sems):
        self.fetch = pltpu.make_async_copy(own, buffer, sems.at[0])
        self.keep = pltpu.make_async_copy(buffer, place, sems.at[1])

    def turn(self):
        self.fetch.wait()
        self.keep.start()


def at_step(step):
    return pl.when(pl.program_id(0) == step)


def forward_kernel(seq_par, group, scale, x_ref, gain_ref, wq_ref, wk_ref, wv_ref, cos_ref, sin_ref, dy_ref, all_ref, q_ref, k_ref, k_rows_ref, v_rows_ref, o_ref, lse_ref, dy_all, v_ref, tile, bounce, w_ref, dy_bounce, tile_sem, bounce_sem, w_sem, dy_sem, send_sem, recv_sem, dy_send, dy_recv):
    block = pl.program_id(0)
    rows = x_ref.shape[0]
    dim = k_ref.shape[0]
    blocks = k_ref.shape[1] // BQ
    wide = group * dim
    block_of = row_place(all_ref, rows)
    dy_place = row_place(dy_all, rows)
    me = lax.axis_index('sp')
    ring = RingGather(seq_par, lambda part: block_of(me, part), block_of, send_sem, recv_sem)
    dy_ring = RingGather(seq_par, row_own(dy_ref, rows), dy_place, dy_send, dy_recv)
    dy_local = Bounce(dy_ref, dy_bounce, dy_place(ring.me, slice(None)), dy_sem)

    def project(rows_ref, source):
        cols = pl.ds(pl.multiple_of(source * rows, rows), rows)
        cos_t = cos_ref[:, cols]
        sin_t = sin_ref[:, cols]
        lin = dot_nt(w_ref[...], rows_ref[...])
        for h in range(group + 2):
            part = lin[h * dim:(h + 1) * dim, :]
            if h < group:
                q_ref[h * dim:(h + 1) * dim, cols] = rotate(part, cos_t, sin_t).astype(BF16)
            elif h == group:
                keys = rotate(part, cos_t, sin_t)
                k_ref[:, cols] = keys.astype(BF16)
                k_rows_ref[cols, :] = keys.T.astype(BF16)
            else:
                v_ref[:, cols] = part.astype(BF16)
                v_rows_ref[cols, :] = part.T.astype(BF16)

    def gathered(source):
        copy = pltpu.make_async_copy(block_of(source, slice(None)), tile, tile_sem)
        copy.start()
        copy.wait()
        project(tile, source)

    @at_step(0)
    def _():
        weights = [
            pltpu.make_async_copy(wq_ref.at[pl.ds(pl.multiple_of(me * wide, wide), wide), :], w_ref.at[:wide, :], w_sem.at[0]),
            pltpu.make_async_copy(wk_ref.at[pl.ds(pl.multiple_of(me * dim, dim), dim), :], w_ref.at[wide:wide + dim, :], w_sem.at[1]),
            pltpu.make_async_copy(wv_ref.at[pl.ds(pl.multiple_of(me * dim, dim), dim), :], w_ref.at[wide + dim:, :], w_sem.at[2]),
        ]
        for copy in weights:
            copy.start()
        keep = pltpu.make_async_copy(bounce, block_of(me, slice(None)), bounce_sem)

        def norm():
            bounce[...] = norm_forward(x_ref[...], gain_ref[...])
            keep.start()
            keep.wait()

        greet(seq_par, norm)
        ring.start()
        for copy in weights:
            copy.wait()
        project(bounce, me)
        ring.p0.wait_recv()
        gathered(ring.partner)
        ring.forward()
        dy_ring.start()
        dy_local.fetch.start()
        ring.relay_near()
        gathered(ring.left)
        gathered(ring.right)
        ring.p1.wait_recv()
        gathered(ring.other(ring.left))
        ring.p2.wait_recv()
        gathered(ring.other(ring.right))
        ring.relay_far()
        gathered(ring.far)
        ring.p3.wait_recv()
        gathered(ring.other(ring.far))
        dy_local.turn()
        ring.finish_sends()

    @at_step(blocks * 5 // 12)
    def _():
        dy_ring.forward()

    @at_step(blocks * 9 // 12)
    def _():
        dy_ring.relay_near()

    cols_q = pl.ds(pl.multiple_of(block * BQ, BQ), BQ)
    q_cat = jnp.concatenate([q_ref[h * dim:(h + 1) * dim, cols_q] for h in range(group)], axis=1)
    wide_q = group * BQ
    factor = scale * LOG2E

    def step(start, carry, masked):
        m_old, l_old, acc = carry
        keys = k_rows_ref[pl.ds(start, BK), :]
        scores = dot(keys, q_cat) * factor
        if masked:
            row = lax.broadcasted_iota(jnp.int32, (BK, wide_q), 0)
            col = lax.broadcasted_iota(jnp.int32, (BK, wide_q), 1) % BQ
            scores = jnp.where(row <= col, scores, -1e30)
        m_new = jnp.maximum(m_old, jnp.max(scores, axis=0, keepdims=True))
        probs = jnp.exp2(scores - m_new)
        alpha = jnp.exp2(m_old - m_new)
        l_new = l_old * alpha + jnp.sum(probs, axis=0, keepdims=True)
        out = dot(v_ref[:, pl.ds(start, BK)], probs.astype(BF16))
        return m_new, l_new, acc * alpha + out

    init = (jnp.full((1, wide_q), -1e30, F32), jnp.zeros((1, wide_q), F32), jnp.zeros((dim, wide_q), F32))
    carry = lax.fori_loop(0, block, lambda i, c: step(pl.multiple_of(i * BK, BK), c, False), init)
    m_fin, l_fin, acc = step(pl.multiple_of(block * BK, BK), carry, True)
    out = (acc / l_fin).astype(BF16)
    lse = m_fin + jnp.log2(l_fin)
    for h in range(group):
        o_ref[h * dim:(h + 1) * dim, :] = out[:, h * BQ:(h + 1) * BQ]
        lse_ref[h:h + 1, :] = lse[:, h * BQ:(h + 1) * BQ]

    @at_step(blocks - 1)
    def _():
        dy_ring.relay_far()
        dy_local.keep.wait()
        dy_ring.finish_recvs()
        dy_ring.finish_sends()


def attention_forward(x_local, gain, wq_t, wk_t, wv_t, cos_t, sin_t, d_out, group, seq_par):
    rows, d_model = x_local.shape
    dim = 2 * cos_t.shape[0]
    seq = rows * seq_par
    scale = dim ** -0.5
    pairs = seq * (seq + BQ) // 2 * group
    hbm = pl.BlockSpec(memory_space=pl.ANY)
    whole = lambda shape: pl.BlockSpec(shape, lambda j: (0, 0))
    shapes = [(group * dim, seq), (dim, seq), (seq, dim), (seq, dim)]
    return pl.pallas_call(
        functools.partial(forward_kernel, seq_par, group, scale),
        grid=(seq // BQ,),
        in_specs=[whole(x_local.shape), whole((1, d_model)), hbm, hbm, hbm, whole(cos_t.shape), whole(sin_t.shape), hbm],
        out_specs=[hbm] + [whole(shape) for shape in shapes] + [
            pl.BlockSpec((group * dim, BQ), lambda j: (0, j)),
            pl.BlockSpec((group, BQ), lambda j: (0, j)),
            hbm,
        ],
        out_shape=[jax.ShapeDtypeStruct((seq, d_model), BF16)] + [jax.ShapeDtypeStruct(shape, BF16) for shape in shapes] + [
            jax.ShapeDtypeStruct((group * dim, seq), BF16),
            jax.ShapeDtypeStruct((group, seq), F32),
            jax.ShapeDtypeStruct((seq, d_model), BF16),
        ],
        scratch_shapes=[
            pltpu.VMEM((dim, seq), BF16),
            pltpu.VMEM((rows, d_model), BF16),
            pltpu.VMEM((rows, d_model), BF16),
            pltpu.VMEM(((group + 2) * dim, d_model), BF16),
            pltpu.VMEM((rows, d_model), BF16),
            pltpu.SemaphoreType.DMA,
            pltpu.SemaphoreType.DMA,
            pltpu.SemaphoreType.DMA((3,)),
            pltpu.SemaphoreType.DMA((2,)),
        ] + GATHER_SEMS + GATHER_SEMS,
        compiler_params=pltpu.CompilerParams(collective_id=1, has_side_effects=True, vmem_limit_bytes=62 << 20),
        cost_estimate=pl.CostEstimate(flops=16 * pairs * dim, transcendentals=pairs, bytes_accessed=8 * seq * d_model),
        name='attn_fwd',
    )(x_local, gain[None], wq_t, wk_t, wv_t, cos_t, sin_t, d_out)


def backward_kernel(seq_par, group, scale, q_ref, dy_ref, wo_ref, o_ref, lse_ref, k_ref, v_ref, kt_ref, cos_ref, sin_ref, own_ref, x_ref, dqb_ref, dkv_ref, y_ref, all_ref, dqa_ref, dk_acc, dv_acc, dq_buf, bounce, wo_buf, wo_sem, o_mine, o_rows, o_sem, bounce_sem, send_sem, recv_sem, dqa_sem, dq_send, dq_recv):
    block = pl.program_id(0)
    blocks = k_ref.shape[0] // BQ
    dim = k_ref.shape[1]
    wide = group * BQ
    factor = scale * LOG2E
    rows = own_ref.shape[0]
    half = dqa_ref.shape[1]
    place = row_place(all_ref, rows)
    ring = RingGather(seq_par, row_own(own_ref, rows), place, send_sem, recv_sem)
    local = Bounce(own_ref, bounce, place(ring.me, slice(None)), bounce_sem)
    dq_place = row_place(dqa_ref, rows)
    dq_ring = RingGather(seq_par, lambda part: dq_place(ring.me, part), dq_place, dq_send, dq_recv)

    @at_step(0)
    def _():
        weights = pltpu.make_async_copy(wo_ref, wo_buf, wo_sem)
        weights.start()
        greet(seq_par)
        ring.start()
        local.fetch.start()
        weights.wait()
        dk_acc[...] = jnp.zeros_like(dk_acc)
        dv_acc[...] = jnp.zeros_like(dv_acc)

    @at_step(1)
    def _():
        local.turn()

    @at_step(blocks * 5 // 12)
    def _():
        ring.forward()

    @at_step(blocks * 8 // 12)
    def _():
        ring.relay_near()
        store = pltpu.make_async_copy(dq_buf.at[:, :half], dq_place(ring.me, slice(None)), dqa_sem)
        store.start()
        store.wait()
        dq_ring.start()

    @at_step(blocks * 10 // 12)
    def _():
        ring.relay_far()

    @at_step(blocks * 11 // 12)
    def _():
        dq_ring.forward()

    do_t = dot_nt(wo_buf[pl.ds(pl.multiple_of(ring.me * rows, rows), rows), :], dy_ref[...]).astype(BF16)
    q_cat = heads_cat(q_ref, group)
    do_cat = jnp.concatenate([do_t[h * dim:(h + 1) * dim, :] for h in range(group)], axis=1)
    o_cat = heads_cat(o_ref, group)
    lse = jnp.concatenate([lse_ref[h:h + 1, :] for h in range(group)], axis=1)
    delta = jnp.sum(do_cat.astype(F32) * o_cat.astype(F32), axis=0, keepdims=True)

    def step(start, dq, masked):
        keys = pl.ds(start, BK)
        scores = dot(k_ref[keys, :], q_cat) * factor
        if masked:
            row = lax.broadcasted_iota(jnp.int32, (BK, wide), 0)
            col = lax.broadcasted_iota(jnp.int32, (BK, wide), 1) % BQ
            scores = jnp.where(row <= col, scores, -1e30)
        probs = jnp.exp2(scores - lse)
        d_probs = dot(v_ref[keys, :], do_cat).astype(BF16).astype(F32)
        d_scores = (probs * (d_probs - delta)).astype(BF16)
        dv_acc[:, keys] += dot_nt(do_cat, probs.astype(BF16))
        dk_acc[:, keys] += dot_nt(q_cat, d_scores)
        return dq + dot(kt_ref[:, keys], d_scores)

    dq = lax.fori_loop(0, block, lambda i, c: step(pl.multiple_of(i * BK, BK), c, False), jnp.zeros((dim, wide), F32))
    dq = step(pl.multiple_of(block * BK, BK), dq, True)
    dq = (dq * scale).astype(BF16).astype(F32)
    cols = pl.ds(pl.multiple_of(block * BQ, BQ), BQ)
    cos_t = cos_ref[:, cols]
    sin_t = sin_ref[:, cols]
    for h in range(group):
        dq_buf[h * dim:(h + 1) * dim, cols] = rotate_back(dq[:, h * BQ:(h + 1) * BQ], cos_t, sin_t).astype(BF16)

    @at_step(blocks - 1)
    def _():
        store = pltpu.make_async_copy(dq_buf.at[:, half:], dqb_ref, dqa_sem)
        store.start()
        dk = (dk_acc[...] * scale).astype(BF16).astype(F32)
        dkv_ref[:dim, :] = rotate_back(dk, cos_ref[...], sin_ref[...]).astype(BF16)
        dkv_ref[dim:, :] = dv_acc[...].astype(BF16)
        dq_ring.relay_near()
        ring.finish_recvs()
        ring.finish_sends()
        local.keep.wait()
        store.wait()
        tokens = x_ref.shape[0]
        fetch = pltpu.make_async_copy(all_ref.at[:, pl.ds(pl.multiple_of(ring.me * tokens, tokens), tokens)], o_mine, o_sem)
        fetch.start()
        fetch.wait()
        o_rows[...] = o_mine[...].T
        d_model = x_ref.shape[1]
        wide_y = math.gcd(d_model, 512)
        for start_y in range(0, d_model, wide_y):
            cols_y = slice(start_y, start_y + wide_y)
            y_ref[:, cols_y] = (x_ref[:, cols_y].astype(F32) + dot(o_rows[...], wo_buf[:, cols_y])).astype(BF16)
        dq_ring.relay_far()
        dq_ring.finish_recvs()
        dq_ring.finish_sends()


def attention_backward(x_local, q_t, dy_all, wo_t, o_t, lse, k_rows, v_rows, k_t, cos_t, sin_t, group, seq_par):
    dim, seq = k_t.shape
    rows, d_model = q_t.shape[0], wo_t.shape[1]
    scale = dim ** -0.5
    half = seq // 2
    pairs = seq * (seq + BQ) // 2 * group
    tile = pl.BlockSpec((rows, BQ), lambda j: (0, j))
    whole = lambda shape: pl.BlockSpec(shape, lambda j: (0, 0))
    hbm = pl.BlockSpec(memory_space=pl.ANY)
    return pl.pallas_call(
        functools.partial(backward_kernel, seq_par, group, scale),
        grid=(seq // BQ,),
        in_specs=[tile, pl.BlockSpec((BQ, d_model), lambda j: (j, 0)), hbm, tile, pl.BlockSpec((group, BQ), lambda j: (0, j)), whole((seq, dim)), whole((seq, dim)), whole((dim, seq)), whole(cos_t.shape), whole(sin_t.shape), hbm, whole(x_local.shape)],
        out_specs=[hbm, whole((2 * dim, seq)), whole(x_local.shape), hbm, hbm],
        out_shape=[
            jax.ShapeDtypeStruct((rows, seq - half), BF16),
            jax.ShapeDtypeStruct((2 * dim, seq), BF16),
            jax.ShapeDtypeStruct(x_local.shape, BF16),
            jax.ShapeDtypeStruct((rows * seq_par, seq), BF16),
            jax.ShapeDtypeStruct((rows * seq_par, half), BF16),
        ],
        scratch_shapes=[pltpu.VMEM((dim, seq), F32), pltpu.VMEM((dim, seq), F32), pltpu.VMEM((rows, seq), BF16), pltpu.VMEM((rows, seq), BF16), pltpu.VMEM(wo_t.shape, BF16), pltpu.SemaphoreType.DMA, pltpu.VMEM((wo_t.shape[0], x_local.shape[0]), BF16), pltpu.VMEM((x_local.shape[0], wo_t.shape[0]), BF16), pltpu.SemaphoreType.DMA, pltpu.SemaphoreType.DMA((2,))] + GATHER_SEMS + [pltpu.SemaphoreType.DMA] + GATHER_SEMS,
        compiler_params=pltpu.CompilerParams(collective_id=3, has_side_effects=True, vmem_limit_bytes=56 << 20),
        cost_estimate=pl.CostEstimate(flops=40 * pairs * dim, transcendentals=pairs, bytes_accessed=12 * group * dim * seq),
        name='attn_bwd',
    )(q_t, dy_all, wo_t, o_t, lse, k_rows, v_rows, k_t, cos_t, sin_t, o_t, x_local)


def tail_gather_kernel(seq_par, dim, o_ref, dy_ref, r_ref, dqb_own, dkv_own, dwo_ref, dk_ref, dv_ref, dqb_ref, dkv_ref, dy_buf, r_buf, dkv_buf, load_sem, dkv_sem, dqb_bounce, dkv_bounce, dqb_local, dkv_local, dqb_send, dqb_recv, dkv_send, dkv_recv):
    tile = pl.program_id(0)
    short = dkv_buf.shape[1]
    dqb_place = row_place(dqb_ref, dqb_own.shape[0])
    dkv_place = row_place(dkv_ref, dkv_own.shape[0])
    dqb = RingGather(seq_par, row_own(dqb_own, dqb_own.shape[0]), dqb_place, dqb_send, dqb_recv)
    dkv = RingGather(seq_par, row_own(dkv_own, dkv_own.shape[0]), dkv_place, dkv_send, dkv_recv)
    keep_dqb = Bounce(dqb_own, dqb_bounce, dqb_place(dqb.me, slice(None)), dqb_local)
    keep_dkv = Bounce(dkv_own, dkv_bounce, dkv_place(dkv.me, slice(None)), dkv_local)
    load_dy = pltpu.make_async_copy(dy_ref, dy_buf, load_sem.at[0])
    load_r = pltpu.make_async_copy(r_ref, r_buf, load_sem.at[1])
    takes = [pltpu.make_async_copy(dkv_ref.at[t * short:(t + 1) * short, :], dkv_buf.at[t], dkv_sem.at[t]) for t in range(dkv_buf.shape[0])]

    @at_step(0)
    def _():
        load_dy.start()
        greet(seq_par)
        dkv.start()
        keep_dqb.fetch.start()
        keep_dkv.fetch.start()
        load_dy.wait()
        load_r.start()

    @at_step(1)
    def _():
        keep_dqb.turn()
        keep_dkv.turn()

    @at_step(2)
    def _():
        dkv.forward()
        dqb.start()

    @at_step(4)
    def _():
        dkv.relay_near()

    @at_step(6)
    def _():
        dkv.relay_far()

    @at_step(TILES)
    def _():
        dqb.forward()
        load_r.wait()
        keep_dkv.keep.wait()
        dkv.finish_recvs()
        for take in takes:
            take.start()

    @at_step(TILES + 2)
    def _():
        dqb.relay_near()

    @pl.when(tile < TILES)
    def _():
        dwo_ref[...] = dot(o_ref[...], dy_buf[...])

    for t, take in enumerate(takes):
        @at_step(TILES + t)
        def _(take=take):
            take.wait()

    @pl.when(tile >= TILES)
    def _():
        both = dot(dkv_buf[tile - TILES], r_buf[...])
        for h in range(dk_ref.shape[0] // dim):
            dk_ref[h * dim:(h + 1) * dim, :] = both[2 * h * dim:(2 * h + 1) * dim, :]
            dv_ref[h * dim:(h + 1) * dim, :] = both[(2 * h + 1) * dim:(2 * h + 2) * dim, :]

    @pl.when(tile == pl.num_programs(0) - 1)
    def _():
        dqb.relay_far()
        keep_dqb.keep.wait()
        dqb.finish_recvs()
        dqb.finish_sends()
        dkv.finish_sends()


TILES = 8


def tail_gather(o_all, dy_all, normed_all, dqb_t, dkv_t, dim, seq_par):
    rows, seq = o_all.shape
    d_model = dy_all.shape[1]
    pair_rows = dkv_t.shape[0] * seq_par
    tall = rows // TILES
    short = math.gcd(pair_rows, 256)
    hbm = pl.BlockSpec(memory_space=pl.ANY)
    first = lambda i: (jnp.minimum(i, TILES - 1), 0)
    second = lambda i: (jnp.maximum(i - TILES, 0), 0)
    return pl.pallas_call(
        functools.partial(tail_gather_kernel, seq_par, dim),
        grid=(TILES + pair_rows // short,),
        in_specs=[pl.BlockSpec((tall, seq), first), hbm, hbm, hbm, hbm],
        out_specs=[pl.BlockSpec((tall, d_model), first), pl.BlockSpec((short // 2, d_model), second), pl.BlockSpec((short // 2, d_model), second), hbm, hbm],
        out_shape=[
            jax.ShapeDtypeStruct((rows, d_model), F32),
            jax.ShapeDtypeStruct((pair_rows // 2, d_model), F32),
            jax.ShapeDtypeStruct((pair_rows // 2, d_model), F32),
            jax.ShapeDtypeStruct((dqb_t.shape[0] * seq_par, dqb_t.shape[1]), BF16),
            jax.ShapeDtypeStruct((pair_rows, seq), BF16),
        ],
        scratch_shapes=[
            pltpu.VMEM(dy_all.shape, BF16),
            pltpu.VMEM(normed_all.shape, BF16),
            pltpu.VMEM((pair_rows // short, short, seq), BF16),
            pltpu.SemaphoreType.DMA((2,)),
            pltpu.SemaphoreType.DMA((pair_rows // short,)),
            pltpu.VMEM(dqb_t.shape, BF16),
            pltpu.VMEM(dkv_t.shape, BF16),
            pltpu.SemaphoreType.DMA((2,)),
            pltpu.SemaphoreType.DMA((2,)),
        ] + GATHER_SEMS + GATHER_SEMS,
        compiler_params=pltpu.CompilerParams(collective_id=5, has_side_effects=True, vmem_limit_bytes=60 << 20),
        cost_estimate=pl.CostEstimate(flops=2 * d_model * seq * (rows + pair_rows), transcendentals=0, bytes_accessed=8 * rows * d_model),
        name='tail_gather',
    )(o_all, dy_all, normed_all, dqb_t, dkv_t)


def finish_kernel(dqa_ref, dqb_ref, dwo_in, dk_in, dv_in, y_in, dx_in, r_ref, dwq_ref, dwo_ref, dk_ref, dv_ref, y_ref, dx_ref, r_buf, load_sem):
    half = dqa_ref.shape[1]
    early = pltpu.make_async_copy(r_ref.at[:half, :], r_buf.at[:half, :], load_sem.at[0])
    late = pltpu.make_async_copy(r_ref.at[half:, :], r_buf.at[half:, :], load_sem.at[1])

    @at_step(0)
    def _():
        early.start()
        late.start()

    def hand_on():
        dwo_ref[...] = dwo_in[...]
        dk_ref[...] = dk_in[...]
        dv_ref[...] = dv_in[...]
        y_ref[...] = y_in[...]
        dx_ref[...] = dx_in[...]

    @at_step(0)
    def _():
        hand_on()
        early.wait()
        dwq_ref[...] = dot(dqa_ref[...], r_buf[:half, :])
        late.wait()
        dwq_ref[...] += dot(dqb_ref[...], r_buf[half:, :])

    @pl.when(pl.program_id(0) > 0)
    def _():
        hand_on()
        dwq_ref[...] = dot(dqa_ref[...], r_buf[:half, :]) + dot(dqb_ref[...], r_buf[half:, :])


def finish_grads(dqa_all, dqb_all, passed, normed_all):
    rows, half = dqa_all.shape
    seq, d_model = normed_all.shape
    band = lambda a: pl.BlockSpec((a.shape[0] // TILES, a.shape[1]), lambda i: (i, 0))
    out = jax.ShapeDtypeStruct((rows, d_model), F32)
    return pl.pallas_call(
        finish_kernel,
        grid=(TILES,),
        in_specs=[band(dqa_all), band(dqb_all)] + [band(p) for p in passed] + [pl.BlockSpec(memory_space=pl.ANY)],
        out_specs=[band(out)] + [band(p) for p in passed],
        out_shape=[out] + [jax.ShapeDtypeStruct(p.shape, p.dtype) for p in passed],
        scratch_shapes=[pltpu.VMEM(normed_all.shape, BF16), pltpu.SemaphoreType.DMA((2,))],
        compiler_params=pltpu.CompilerParams(vmem_limit_bytes=60 << 20),
        cost_estimate=pl.CostEstimate(flops=2 * d_model * rows * seq, transcendentals=0, bytes_accessed=16 * rows * d_model),
        name='finish_grads',
    )(dqa_all, dqb_all, *passed, normed_all)


def input_grad_kernel(seq_par, dqa_ref, dqb_ref, dkv_ref, wq_ref, wk_ref, wv_ref, x_ref, dy_ref, gain_ref, dx_ref, dgain_ref, dq_buf, dk_buf, dv_buf, wq_buf, wk_buf, wv_buf, acc, part, slots, act_sem, w_sem, send_sem, recv_sem):
    me = lax.axis_index('sp')
    tokens, d_model = x_ref.shape
    half = dqa_ref.shape[1]
    barrier = pltpu.get_barrier_semaphore()
    for step in range(1, seq_par):
        pl.semaphore_signal(barrier, inc=1, device_id={'sp': lax.rem(me + step, seq_par)}, device_id_type=pl.DeviceIdType.MESH)
    low = me * tokens < half
    first = pl.multiple_of(jnp.where(low, me * tokens, 0), 128)
    second = pl.multiple_of(jnp.where(low, 0, me * tokens - half), 128)
    cols = pl.ds(pl.multiple_of(me * tokens, tokens), tokens)
    from_a = pltpu.make_async_copy(dqa_ref.at[:, pl.ds(first, tokens)], dq_buf, act_sem.at[0])
    from_b = pltpu.make_async_copy(dqb_ref.at[:, pl.ds(second, tokens)], dq_buf, act_sem.at[0])

    @pl.when(low)
    def _():
        from_a.start()

    @pl.when(jnp.logical_not(low))
    def _():
        from_b.start()

    take_k = pltpu.make_async_copy(dkv_ref.at[:, 0, :, cols], dk_buf, act_sem.at[1])
    take_v = pltpu.make_async_copy(dkv_ref.at[:, 1, :, cols], dv_buf, act_sem.at[2])
    take_k.start()
    take_v.start()
    chunk = wq_buf.shape[0] // 4
    loads = [pltpu.make_async_copy(wq_ref.at[c * chunk:(c + 1) * chunk, :], wq_buf.at[c * chunk:(c + 1) * chunk, :], w_sem.at[c]) for c in range(4)]
    loads += [pltpu.make_async_copy(wk_ref, wk_buf, w_sem.at[4]), pltpu.make_async_copy(wv_ref, wv_buf, w_sem.at[5])]
    for copy in loads:
        copy.start()
    from_a.wait()
    for c in range(4):
        loads[c].wait()
        term = dot(dq_buf[c * chunk:(c + 1) * chunk, :].T, wq_buf[c * chunk:(c + 1) * chunk, :])
        if c == 0:
            acc[...] = term
        else:
            acc[...] += term
    take_k.wait()
    take_v.wait()
    loads[4].wait()
    loads[5].wait()
    acc[...] += dot(dk_buf[...].reshape(wk_buf.shape[0], tokens).T, wk_buf[...])
    acc[...] += dot(dv_buf[...].reshape(wv_buf.shape[0], tokens).T, wv_buf[...])
    d_normed = acc[...].astype(BF16).astype(F32)
    acc[...] = d_normed
    x_f32 = x_ref[...].astype(F32)
    inv_rms = lax.rsqrt(jnp.mean(x_f32 * x_f32, axis=-1, keepdims=True) + NORM_EPS)
    part[...] = jnp.sum(d_normed * (x_f32 * inv_rms), axis=0, keepdims=True)
    dots = jnp.mean(acc[...] * gain_ref[...] * (x_ref[...].astype(F32) * inv_rms), axis=-1, keepdims=True)
    pl.semaphore_wait(barrier, seq_par - 1)
    copies = []
    for step in range(1, seq_par):
        copies.append(pltpu.make_async_remote_copy(src_ref=part, dst_ref=slots.at[me], send_sem=send_sem.at[step], recv_sem=recv_sem.at[step], device_id={'sp': lax.rem(me + step, seq_par)}, device_id_type=pl.DeviceIdType.MESH))
        copies[-1].start()
    slots[me] = part[...]
    x_hat = x_ref[...].astype(F32) * inv_rms
    dx_ref[...] = (dy_ref[...].astype(F32) + inv_rms * (acc[...] * gain_ref[...] - x_hat * dots)).astype(BF16)
    for copy in copies:
        copy.wait_recv()
    total = slots[0]
    for step in range(1, seq_par):
        total = total + slots[step]
    dgain_ref[...] = total
    for copy in copies:
        copy.wait_send()


def input_grad(dqa_all, dqb_all, dkv_all, wq_t, wk_t, wv_t, x_local, dy_local, gain, dim, seq_par):
    tokens, d_model = x_local.shape
    num_kv = wk_t.shape[0] // dim
    seq = dkv_all.shape[1]
    vmem = pl.BlockSpec(memory_space=pltpu.VMEM)
    hbm = pl.BlockSpec(memory_space=pl.ANY)
    return pl.pallas_call(
        functools.partial(input_grad_kernel, seq_par),
        in_specs=[hbm] * 6 + [vmem] * 3,
        out_specs=[vmem, vmem],
        out_shape=[jax.ShapeDtypeStruct(x_local.shape, BF16), jax.ShapeDtypeStruct((1, d_model), F32)],
        scratch_shapes=[
            pltpu.VMEM((wq_t.shape[0], tokens), BF16),
            pltpu.VMEM((num_kv, dim, tokens), BF16),
            pltpu.VMEM((num_kv, dim, tokens), BF16),
            pltpu.VMEM(wq_t.shape, BF16),
            pltpu.VMEM(wk_t.shape, BF16),
            pltpu.VMEM(wv_t.shape, BF16),
            pltpu.VMEM((tokens, d_model), F32),
            pltpu.VMEM((1, d_model), F32),
            pltpu.VMEM((seq_par, 1, d_model), F32),
            pltpu.SemaphoreType.DMA((3,)),
            pltpu.SemaphoreType.DMA((6,)),
            pltpu.SemaphoreType.DMA((seq_par,)),
            pltpu.SemaphoreType.DMA((seq_par,)),
        ],
        compiler_params=pltpu.CompilerParams(collective_id=4, has_side_effects=True, vmem_limit_bytes=56 << 20),
        cost_estimate=pl.CostEstimate(flops=2 * tokens * d_model * (wq_t.shape[0] + 2 * wk_t.shape[0]), transcendentals=0, bytes_accessed=2 * d_model * (wq_t.shape[0] + 2 * wk_t.shape[0])),
        name='input_grad',
    )(dqa_all, dqb_all, dkv_all.reshape(num_kv, 2, dim, seq), wq_t, wk_t, wv_t, x_local, dy_local, gain[None])


def solution(mesh):
    seq_par = mesh.shape['sp']

    def local_step(x_local, dy_local, gain, w_q, w_k, w_v, w_o):
        _, seq_loc, d_model = x_local.shape
        num_q, dim = w_q.shape[1], w_q.shape[2]
        num_kv = w_k.shape[1]
        group = num_q // num_kv
        if num_kv != seq_par or seq_par % 4:
            raise ValueError('unsupported mesh')
        seq = seq_loc * seq_par
        x_local = x_local[0]
        dy_local = dy_local[0]
        wq_t = jnp.transpose(w_q, (1, 2, 0)).reshape(num_q * dim, d_model)
        wk_t = jnp.transpose(w_k, (1, 2, 0)).reshape(num_kv * dim, d_model)
        wv_t = jnp.transpose(w_v, (1, 2, 0)).reshape(num_kv * dim, d_model)
        wo_t = w_o.reshape(num_q * dim, d_model)

        cos_t, sin_t = rope_tables(jnp.arange(seq, dtype=F32), dim)
        normed_all, q_t, k_t, k_rows, v_rows, o_t, lse, dy_all = attention_forward(x_local, gain, wq_t, wk_t, wv_t, cos_t, sin_t, dy_local, group, seq_par)
        dqb_t, dkv_t, y_out, o_all, dqa_all = attention_backward(x_local, q_t, dy_all, wo_t, o_t, lse, k_rows, v_rows, k_t, cos_t, sin_t, group, seq_par)
        d_wo, d_wk, d_wv, dqb_all, dkv_all = tail_gather(o_all, dy_all, normed_all, dqb_t, dkv_t, dim, seq_par)
        d_x, d_gain = input_grad(dqa_all, dqb_all, dkv_all, wq_t, wk_t, wv_t, x_local, dy_local, gain, dim, seq_par)
        d_wq, d_wo, d_wk, d_wv, y_out, d_x = finish_grads(dqa_all, dqb_all, [d_wo, d_wk, d_wv, y_out, d_x], normed_all)
        unflat = lambda g, heads: jnp.transpose(g.reshape(heads, dim, d_model), (2, 0, 1))
        return y_out[None], d_x[None], unflat(d_wq, num_q), unflat(d_wk, num_kv), unflat(d_wv, num_kv), d_wo.reshape(num_q, dim, d_model), d_gain[0]

    specs_in = (P('dp', 'sp', None), P('dp', 'sp', None), P(None), P(None, None, None), P(None, None, None), P(None, None, None), P(None, None, None))
    specs_out = (P('dp', 'sp', None), P('dp', 'sp', None), P('dp', None, None), P('dp', None, None), P('dp', None, None), P('dp', None, None), P('dp'))
    return jax.shard_map(local_step, mesh=mesh, in_specs=specs_in, out_specs=specs_out, check_vma=False)
```

```python
import functools
import math
import jax
import jax.numpy as jnp
from jax import lax
from jax.experimental import pallas as pl
from jax.experimental.pallas import tpu as pltpu
from jax.sharding import PartitionSpec as P

ROPE_BASE = 1000000.0
NORM_EPS = 1e-5
LOG2E = math.log2(math.e)
BQ = 256
BK = 256
NT = (((1,), (1,)), ((), ()))
TN = (((0,), (0,)), ((), ()))
F32 = jnp.float32
BF16 = jnp.bfloat16


def rope_tables(positions, head_dim):
    half = head_dim // 2
    inv_freq = ROPE_BASE ** (-2.0 * jnp.arange(half, dtype=F32) / head_dim)
    angle = inv_freq[:, None] * positions[None, :]
    return jnp.cos(angle), jnp.sin(angle)


def rotate(vals, cos_t, sin_t):
    half = vals.shape[-2] // 2
    first = vals[..., :half, :]
    second = vals[..., half:, :]
    return jnp.concatenate([first * cos_t - second * sin_t, second * cos_t + first * sin_t], axis=-2)


def rotate_back(vals, cos_t, sin_t):
    half = vals.shape[-2] // 2
    first = vals[..., :half, :]
    second = vals[..., half:, :]
    return jnp.concatenate([first * cos_t + second * sin_t, second * cos_t - first * sin_t], axis=-2)


def norm_forward(x_local, gain):
    x_f32 = x_local.astype(F32)
    inv_rms = lax.rsqrt(jnp.mean(x_f32 * x_f32, axis=-1, keepdims=True) + NORM_EPS)
    return (x_f32 * inv_rms * gain).astype(BF16)


def dot(a, b):
    return jnp.dot(a, b, preferred_element_type=F32)


def dot_nt(a, b):
    return lax.dot_general(a, b, NT, preferred_element_type=F32)


def heads_cat(ref, num):
    dim = ref.shape[0] // num
    return jnp.concatenate([ref[h * dim:(h + 1) * dim, :] for h in range(num)], axis=1)


class RingGather:
    def __init__(self, seq_par, own, place, send_sem, recv_sem):
        me = lax.axis_index('sp')
        self.me = me
        self.partner = me + 1 - 2 * lax.rem(me, 2)
        self.right = lax.rem(me + 2, seq_par)
        self.left = lax.rem(me + seq_par - 2, seq_par)
        self.far = lax.rem(me + 4, seq_par)
        self.other = lambda b: b + 1 - 2 * lax.rem(b, 2)
        both = slice(None)

        def remote(num, src, dst, to):
            return pltpu.make_async_remote_copy(src_ref=src, dst_ref=dst, send_sem=send_sem.at[num], recv_sem=recv_sem.at[num], device_id={'sp': to}, device_id_type=pl.DeviceIdType.MESH)

        self.r1 = remote(0, own(0), place(me, 0), self.right)
        self.l1 = remote(1, own(1), place(me, 1), self.left)
        self.r2 = remote(2, own(1), place(me, 1), self.right)
        self.l2 = remote(3, own(0), place(me, 0), self.left)
        self.p0 = remote(4, own(both), place(me, both), self.partner)
        self.r3 = remote(5, place(self.left, 0), place(self.left, 0), self.right)
        self.l3 = remote(6, place(self.right, 1), place(self.right, 1), self.left)
        self.p1 = remote(7, place(self.left, both), place(self.left, both), self.partner)
        self.p2 = remote(8, place(self.right, both), place(self.right, both), self.partner)
        self.p3 = remote(9, place(self.far, both), place(self.far, both), self.partner)

    def start(self):
        self.r1.start()
        self.l1.start()
        self.r2.start()
        self.l2.start()
        self.p0.start()

    def forward(self):
        self.r1.wait_recv()
        self.r3.start()
        self.l1.wait_recv()
        self.l3.start()

    def relay_near(self):
        self.r2.wait_recv()
        self.p1.start()
        self.l2.wait_recv()
        self.p2.start()

    def relay_far(self):
        self.r3.wait_recv()
        self.l3.wait_recv()
        self.p3.start()

    def finish_sends(self):
        for copy in (self.r1, self.l1, self.r2, self.l2, self.p0, self.r3, self.l3, self.p1, self.p2, self.p3):
            copy.wait_send()

    def finish_recvs(self):
        for copy in (self.p0, self.p1, self.p2, self.p3):
            copy.wait_recv()


GATHER_SEMS = [pltpu.SemaphoreType.DMA((10,)), pltpu.SemaphoreType.DMA((10,))]


def greet(seq_par, meanwhile=None):
    me = lax.axis_index('sp')
    barrier = pltpu.get_barrier_semaphore()
    for peer in (me + 1 - 2 * lax.rem(me, 2), lax.rem(me + 2, seq_par), lax.rem(me + seq_par - 2, seq_par)):
        pl.semaphore_signal(barrier, inc=1, device_id={'sp': peer}, device_id_type=pl.DeviceIdType.MESH)
    if meanwhile is not None:
        meanwhile()
    pl.semaphore_wait(barrier, 3)


def greet_all(seq_par):
    me = lax.axis_index('sp')
    barrier = pltpu.get_barrier_semaphore()
    for step in range(1, seq_par):
        pl.semaphore_signal(barrier, inc=1, device_id={'sp': lax.rem(me + step, seq_par)}, device_id_type=pl.DeviceIdType.MESH)
    pl.semaphore_wait(barrier, seq_par - 1)


def row_place(ref, rows):
    half = rows // 2

    def place(block, part):
        if isinstance(part, int):
            return ref.at[pl.ds(pl.multiple_of(block * rows + part * half, half), half), :]
        return ref.at[pl.ds(pl.multiple_of(block * rows, rows), rows), :]

    return place


def row_own(ref, rows):
    half = rows // 2

    def own(part):
        if isinstance(part, int):
            return ref.at[part * half:(part + 1) * half, :]
        return ref

    return own


class Bounce:
    def __init__(self, own, buffer, place, sems):
        self.fetch = pltpu.make_async_copy(own, buffer, sems.at[0])
        self.keep = pltpu.make_async_copy(buffer, place, sems.at[1])

    def turn(self):
        self.fetch.wait()
        self.keep.start()


def at_step(step):
    return pl.when(pl.program_id(0) == step)


def forward_kernel(seq_par, group, scale, x_ref, gain_ref, wq_ref, wk_ref, wv_ref, cos_ref, sin_ref, dy_ref, all_ref, q_ref, k_ref, k_rows_ref, v_rows_ref, o_ref, lse_ref, dy_all, v_ref, tile, bounce, w_ref, dy_bounce, tile_sem, bounce_sem, w_sem, dy_sem, send_sem, recv_sem, dy_send, dy_recv):
    block = pl.program_id(0)
    rows = x_ref.shape[0]
    dim = k_ref.shape[0]
    blocks = k_ref.shape[1] // BQ
    wide = group * dim
    block_of = row_place(all_ref, rows)
    dy_place = row_place(dy_all, rows)
    me = lax.axis_index('sp')
    ring = RingGather(seq_par, lambda part: block_of(me, part), block_of, send_sem, recv_sem)
    dy_ring = RingGather(seq_par, row_own(dy_ref, rows), dy_place, dy_send, dy_recv)
    dy_local = Bounce(dy_ref, dy_bounce, dy_place(ring.me, slice(None)), dy_sem)

    def project(rows_ref, source):
        cols = pl.ds(pl.multiple_of(source * rows, rows), rows)
        cos_t = cos_ref[:, cols]
        sin_t = sin_ref[:, cols]
        lin = dot_nt(w_ref[...], rows_ref[...])
        for h in range(group + 2):
            part = lin[h * dim:(h + 1) * dim, :]
            if h < group:
                q_ref[h * dim:(h + 1) * dim, cols] = rotate(part, cos_t, sin_t).astype(BF16)
            elif h == group:
                keys = rotate(part, cos_t, sin_t)
                k_ref[:, cols] = keys.astype(BF16)
                k_rows_ref[cols, :] = keys.T.astype(BF16)
            else:
                v_ref[:, cols] = part.astype(BF16)
                v_rows_ref[cols, :] = part.T.astype(BF16)

    def gathered(source):
        copy = pltpu.make_async_copy(block_of(source, slice(None)), tile, tile_sem)
        copy.start()
        copy.wait()
        project(tile, source)

    @at_step(0)
    def _():
        weights = [
            pltpu.make_async_copy(wq_ref.at[pl.ds(pl.multiple_of(me * wide, wide), wide), :], w_ref.at[:wide, :], w_sem.at[0]),
            pltpu.make_async_copy(wk_ref.at[pl.ds(pl.multiple_of(me * dim, dim), dim), :], w_ref.at[wide:wide + dim, :], w_sem.at[1]),
            pltpu.make_async_copy(wv_ref.at[pl.ds(pl.multiple_of(me * dim, dim), dim), :], w_ref.at[wide + dim:, :], w_sem.at[2]),
        ]
        for copy in weights:
            copy.start()
        keep = pltpu.make_async_copy(bounce, block_of(me, slice(None)), bounce_sem)

        def norm():
            bounce[...] = norm_forward(x_ref[...], gain_ref[...])
            keep.start()
            keep.wait()

        greet(seq_par, norm)
        ring.start()
        for copy in weights:
            copy.wait()
        project(bounce, me)
        ring.p0.wait_recv()
        gathered(ring.partner)
        ring.forward()
        dy_ring.start()
        dy_local.fetch.start()
        ring.relay_near()
        gathered(ring.left)
        gathered(ring.right)
        ring.p1.wait_recv()
        gathered(ring.other(ring.left))
        ring.p2.wait_recv()
        gathered(ring.other(ring.right))
        ring.relay_far()
        gathered(ring.far)
        ring.p3.wait_recv()
        gathered(ring.other(ring.far))
        dy_local.turn()
        ring.finish_sends()

    @at_step(blocks * 5 // 12)
    def _():
        dy_ring.forward()

    @at_step(blocks * 9 // 12)
    def _():
        dy_ring.relay_near()

    cols_q = pl.ds(pl.multiple_of(block * BQ, BQ), BQ)
    q_cat = jnp.concatenate([q_ref[h * dim:(h + 1) * dim, cols_q] for h in range(group)], axis=1)
    wide_q = group * BQ
    factor = scale * LOG2E

    def step(start, carry, masked):
        m_old, l_old, acc = carry
        keys = k_rows_ref[pl.ds(start, BK), :]
        scores = dot(keys, q_cat) * factor
        if masked:
            row = lax.broadcasted_iota(jnp.int32, (BK, wide_q), 0)
            col = lax.broadcasted_iota(jnp.int32, (BK, wide_q), 1) % BQ
            scores = jnp.where(row <= col, scores, -1e30)
        m_new = jnp.maximum(m_old, jnp.max(scores, axis=0, keepdims=True))
        probs = jnp.exp2(scores - m_new)
        alpha = jnp.exp2(m_old - m_new)
        l_new = l_old * alpha + jnp.sum(probs, axis=0, keepdims=True)
        out = dot(v_ref[:, pl.ds(start, BK)], probs.astype(BF16))
        return m_new, l_new, acc * alpha + out

    init = (jnp.full((1, wide_q), -1e30, F32), jnp.zeros((1, wide_q), F32), jnp.zeros((dim, wide_q), F32))
    carry = lax.fori_loop(0, block, lambda i, c: step(pl.multiple_of(i * BK, BK), c, False), init)
    m_fin, l_fin, acc = step(pl.multiple_of(block * BK, BK), carry, True)
    out = (acc / l_fin).astype(BF16)
    lse = m_fin + jnp.log2(l_fin)
    for h in range(group):
        o_ref[h * dim:(h + 1) * dim, :] = out[:, h * BQ:(h + 1) * BQ]
        lse_ref[h:h + 1, :] = lse[:, h * BQ:(h + 1) * BQ]

    @at_step(blocks - 1)
    def _():
        dy_ring.relay_far()
        dy_local.keep.wait()
        dy_ring.finish_recvs()
        dy_ring.finish_sends()


def attention_forward(x_local, gain, wq_t, wk_t, wv_t, cos_t, sin_t, d_out, group, seq_par):
    rows, d_model = x_local.shape
    dim = 2 * cos_t.shape[0]
    seq = rows * seq_par
    scale = dim ** -0.5
    pairs = seq * (seq + BQ) // 2 * group
    hbm = pl.BlockSpec(memory_space=pl.ANY)
    whole = lambda shape: pl.BlockSpec(shape, lambda j: (0, 0))
    shapes = [(group * dim, seq), (dim, seq), (seq, dim), (seq, dim)]
    return pl.pallas_call(
        functools.partial(forward_kernel, seq_par, group, scale),
        grid=(seq // BQ,),
        in_specs=[whole(x_local.shape), whole((1, d_model)), hbm, hbm, hbm, whole(cos_t.shape), whole(sin_t.shape), hbm],
        out_specs=[hbm] + [whole(shape) for shape in shapes] + [
            pl.BlockSpec((group * dim, BQ), lambda j: (0, j)),
            pl.BlockSpec((group, BQ), lambda j: (0, j)),
            hbm,
        ],
        out_shape=[jax.ShapeDtypeStruct((seq, d_model), BF16)] + [jax.ShapeDtypeStruct(shape, BF16) for shape in shapes] + [
            jax.ShapeDtypeStruct((group * dim, seq), BF16),
            jax.ShapeDtypeStruct((group, seq), F32),
            jax.ShapeDtypeStruct((seq, d_model), BF16),
        ],
        scratch_shapes=[
            pltpu.VMEM((dim, seq), BF16),
            pltpu.VMEM((rows, d_model), BF16),
            pltpu.VMEM((rows, d_model), BF16),
            pltpu.VMEM(((group + 2) * dim, d_model), BF16),
            pltpu.VMEM((rows, d_model), BF16),
            pltpu.SemaphoreType.DMA,
            pltpu.SemaphoreType.DMA,
            pltpu.SemaphoreType.DMA((3,)),
            pltpu.SemaphoreType.DMA((2,)),
        ] + GATHER_SEMS + GATHER_SEMS,
        compiler_params=pltpu.CompilerParams(collective_id=1, has_side_effects=True, vmem_limit_bytes=62 << 20),
        cost_estimate=pl.CostEstimate(flops=16 * pairs * dim, transcendentals=pairs, bytes_accessed=8 * seq * d_model),
        name='attn_fwd',
    )(x_local, gain[None], wq_t, wk_t, wv_t, cos_t, sin_t, d_out)


def backward_kernel(seq_par, group, scale, q_ref, dy_ref, wo_ref, o_ref, lse_ref, k_ref, v_ref, kt_ref, cos_ref, sin_ref, own_ref, x_ref, dqb_ref, dkv_ref, y_ref, all_ref, dqa_ref, dk_acc, dv_acc, dq_buf, bounce, wo_buf, wo_sem, o_mine, o_rows, o_sem, bounce_sem, send_sem, recv_sem, dqa_sem, dq_send, dq_recv):
    block = pl.program_id(0)
    blocks = k_ref.shape[0] // BQ
    dim = k_ref.shape[1]
    wide = group * BQ
    factor = scale * LOG2E
    rows = own_ref.shape[0]
    half = dqa_ref.shape[1]
    place = row_place(all_ref, rows)
    ring = RingGather(seq_par, row_own(own_ref, rows), place, send_sem, recv_sem)
    local = Bounce(own_ref, bounce, place(ring.me, slice(None)), bounce_sem)
    dq_place = row_place(dqa_ref, rows)
    dq_ring = RingGather(seq_par, lambda part: dq_place(ring.me, part), dq_place, dq_send, dq_recv)

    @at_step(0)
    def _():
        weights = pltpu.make_async_copy(wo_ref, wo_buf, wo_sem)
        weights.start()
        greet(seq_par)
        ring.start()
        local.fetch.start()
        weights.wait()
        dk_acc[...] = jnp.zeros_like(dk_acc)
        dv_acc[...] = jnp.zeros_like(dv_acc)

    @at_step(1)
    def _():
        local.turn()

    @at_step(blocks * 5 // 12)
    def _():
        ring.forward()

    @at_step(blocks * 8 // 12)
    def _():
        ring.relay_near()
        store = pltpu.make_async_copy(dq_buf.at[:, :half], dq_place(ring.me, slice(None)), dqa_sem)
        store.start()
        store.wait()
        dq_ring.start()

    @at_step(blocks * 10 // 12)
    def _():
        ring.relay_far()

    @at_step(blocks * 11 // 12)
    def _():
        dq_ring.forward()

    do_t = dot_nt(wo_buf[pl.ds(pl.multiple_of(ring.me * rows, rows), rows), :], dy_ref[...]).astype(BF16)
    q_cat = heads_cat(q_ref, group)
    do_cat = jnp.concatenate([do_t[h * dim:(h + 1) * dim, :] for h in range(group)], axis=1)
    o_cat = heads_cat(o_ref, group)
    lse = jnp.concatenate([lse_ref[h:h + 1, :] for h in range(group)], axis=1)
    delta = jnp.sum(do_cat.astype(F32) * o_cat.astype(F32), axis=0, keepdims=True)

    def step(start, dq, masked):
        keys = pl.ds(start, BK)
        scores = dot(k_ref[keys, :], q_cat) * factor
        if masked:
            row = lax.broadcasted_iota(jnp.int32, (BK, wide), 0)
            col = lax.broadcasted_iota(jnp.int32, (BK, wide), 1) % BQ
            scores = jnp.where(row <= col, scores, -1e30)
        probs = jnp.exp2(scores - lse)
        d_probs = dot(v_ref[keys, :], do_cat).astype(BF16).astype(F32)
        d_scores = (probs * (d_probs - delta)).astype(BF16)
        dv_acc[:, keys] += dot_nt(do_cat, probs.astype(BF16))
        dk_acc[:, keys] += dot_nt(q_cat, d_scores)
        return dq + dot(kt_ref[:, keys], d_scores)

    dq = lax.fori_loop(0, block, lambda i, c: step(pl.multiple_of(i * BK, BK), c, False), jnp.zeros((dim, wide), F32))
    dq = step(pl.multiple_of(block * BK, BK), dq, True)
    dq = (dq * scale).astype(BF16).astype(F32)
    cols = pl.ds(pl.multiple_of(block * BQ, BQ), BQ)
    cos_t = cos_ref[:, cols]
    sin_t = sin_ref[:, cols]
    for h in range(group):
        dq_buf[h * dim:(h + 1) * dim, cols] = rotate_back(dq[:, h * BQ:(h + 1) * BQ], cos_t, sin_t).astype(BF16)

    @at_step(blocks - 1)
    def _():
        store = pltpu.make_async_copy(dq_buf.at[:, half:], dqb_ref, dqa_sem)
        store.start()
        dk = (dk_acc[...] * scale).astype(BF16).astype(F32)
        dkv_ref[:dim, :] = rotate_back(dk, cos_ref[...], sin_ref[...]).astype(BF16)
        dkv_ref[dim:, :] = dv_acc[...].astype(BF16)
        dq_ring.relay_near()
        ring.finish_recvs()
        ring.finish_sends()
        local.keep.wait()
        store.wait()
        tokens = x_ref.shape[0]
        fetch = pltpu.make_async_copy(all_ref.at[:, pl.ds(pl.multiple_of(ring.me * tokens, tokens), tokens)], o_mine, o_sem)
        fetch.start()
        fetch.wait()
        o_rows[...] = o_mine[...].T
        d_model = x_ref.shape[1]
        wide_y = math.gcd(d_model, 512)
        for start_y in range(0, d_model, wide_y):
            cols_y = slice(start_y, start_y + wide_y)
            y_ref[:, cols_y] = (x_ref[:, cols_y].astype(F32) + dot(o_rows[...], wo_buf[:, cols_y])).astype(BF16)
        dq_ring.relay_far()
        dq_ring.finish_recvs()
        dq_ring.finish_sends()


def attention_backward(x_local, q_t, dy_all, wo_t, o_t, lse, k_rows, v_rows, k_t, cos_t, sin_t, group, seq_par):
    dim, seq = k_t.shape
    rows, d_model = q_t.shape[0], wo_t.shape[1]
    scale = dim ** -0.5
    half = seq // 2
    pairs = seq * (seq + BQ) // 2 * group
    tile = pl.BlockSpec((rows, BQ), lambda j: (0, j))
    whole = lambda shape: pl.BlockSpec(shape, lambda j: (0, 0))
    hbm = pl.BlockSpec(memory_space=pl.ANY)
    return pl.pallas_call(
        functools.partial(backward_kernel, seq_par, group, scale),
        grid=(seq // BQ,),
        in_specs=[tile, pl.BlockSpec((BQ, d_model), lambda j: (j, 0)), hbm, tile, pl.BlockSpec((group, BQ), lambda j: (0, j)), whole((seq, dim)), whole((seq, dim)), whole((dim, seq)), whole(cos_t.shape), whole(sin_t.shape), hbm, whole(x_local.shape)],
        out_specs=[hbm, whole((2 * dim, seq)), whole(x_local.shape), hbm, hbm],
        out_shape=[
            jax.ShapeDtypeStruct((rows, seq - half), BF16),
            jax.ShapeDtypeStruct((2 * dim, seq), BF16),
            jax.ShapeDtypeStruct(x_local.shape, BF16),
            jax.ShapeDtypeStruct((rows * seq_par, seq), BF16),
            jax.ShapeDtypeStruct((rows * seq_par, half), BF16),
        ],
        scratch_shapes=[pltpu.VMEM((dim, seq), F32), pltpu.VMEM((dim, seq), F32), pltpu.VMEM((rows, seq), BF16), pltpu.VMEM((rows, seq), BF16), pltpu.VMEM(wo_t.shape, BF16), pltpu.SemaphoreType.DMA, pltpu.VMEM((wo_t.shape[0], x_local.shape[0]), BF16), pltpu.VMEM((x_local.shape[0], wo_t.shape[0]), BF16), pltpu.SemaphoreType.DMA, pltpu.SemaphoreType.DMA((2,))] + GATHER_SEMS + [pltpu.SemaphoreType.DMA] + GATHER_SEMS,
        compiler_params=pltpu.CompilerParams(collective_id=3, has_side_effects=True, vmem_limit_bytes=56 << 20),
        cost_estimate=pl.CostEstimate(flops=40 * pairs * dim, transcendentals=pairs, bytes_accessed=12 * group * dim * seq),
        name='attn_bwd',
    )(q_t, dy_all, wo_t, o_t, lse, k_rows, v_rows, k_t, cos_t, sin_t, o_t, x_local)


def tail_gather_kernel(seq_par, dim, o_ref, dy_ref, r_ref, dqb_own, dkv_own, dqa_ref, wq_ref, wk_ref, wv_ref, x_ref, dyl_ref, gain_ref, dwo_ref, dk_ref, dv_ref, dqb_ref, dkv_ref, dx_ref, dgain_ref, dy_buf, r_buf, dkv_buf, load_sem, dkv_sem, dqb_bounce, dkv_bounce, dqb_local, dkv_local, dqb_send, dqb_recv, dkv_send, dkv_recv, dq_buf, acc, part, slots, w_sem, dq_sem, gain_send, gain_recv):
    tile = pl.program_id(0)
    short = dkv_buf.shape[1]
    dqb_place = row_place(dqb_ref, dqb_own.shape[0])
    dkv_place = row_place(dkv_ref, dkv_own.shape[0])
    dqb = RingGather(seq_par, row_own(dqb_own, dqb_own.shape[0]), dqb_place, dqb_send, dqb_recv)
    dkv = RingGather(seq_par, row_own(dkv_own, dkv_own.shape[0]), dkv_place, dkv_send, dkv_recv)
    keep_dqb = Bounce(dqb_own, dqb_bounce, dqb_place(dqb.me, slice(None)), dqb_local)
    keep_dkv = Bounce(dkv_own, dkv_bounce, dkv_place(dkv.me, slice(None)), dkv_local)
    load_dy = pltpu.make_async_copy(dy_ref, dy_buf, load_sem.at[0])
    load_r = pltpu.make_async_copy(r_ref, r_buf, load_sem.at[1])
    takes = [pltpu.make_async_copy(dkv_ref.at[t * short:(t + 1) * short, :], dkv_buf.at[t], dkv_sem.at[t]) for t in range(dkv_buf.shape[0])]

    me = dqb.me
    tokens = x_ref.shape[0]
    half = dqa_ref.shape[1]
    ends = [wq_ref.shape[0], wq_ref.shape[0] + wk_ref.shape[0]]
    weights = [
        pltpu.make_async_copy(wq_ref, dy_buf.at[:ends[0], :], w_sem.at[0]),
        pltpu.make_async_copy(wk_ref, dy_buf.at[ends[0]:ends[1], :], w_sem.at[1]),
        pltpu.make_async_copy(wv_ref, dy_buf.at[ends[1]:, :], w_sem.at[2]),
    ]

    @at_step(0)
    def _():
        load_dy.start()
        greet_all(seq_par)
        dkv.start()
        keep_dqb.fetch.start()
        keep_dkv.fetch.start()
        load_dy.wait()
        load_r.start()

    @at_step(1)
    def _():
        keep_dqb.turn()
        keep_dkv.turn()

    @at_step(2)
    def _():
        dkv.forward()
        dqb.start()

    @at_step(4)
    def _():
        dkv.relay_near()

    @at_step(6)
    def _():
        dkv.relay_far()

    @at_step(TILES)
    def _():
        dqb.forward()
        load_r.wait()
        keep_dkv.keep.wait()
        dkv.finish_recvs()
        for take in takes:
            take.start()
        for copy in weights:
            copy.start()

    @at_step(TILES + 2)
    def _():
        dqb.relay_near()

    @pl.when(tile < TILES)
    def _():
        dwo_ref[...] = dot(o_ref[...], dy_buf[...])

    for t, take in enumerate(takes):
        @at_step(TILES + t)
        def _(take=take):
            take.wait()

    @pl.when(tile >= TILES)
    def _():
        both = dot(dkv_buf[tile - TILES], r_buf[...])
        for h in range(dk_ref.shape[0] // dim):
            dk_ref[h * dim:(h + 1) * dim, :] = both[2 * h * dim:(2 * h + 1) * dim, :]
            dv_ref[h * dim:(h + 1) * dim, :] = both[(2 * h + 1) * dim:(2 * h + 2) * dim, :]

    @pl.when(tile == pl.num_programs(0) - 1)
    def _():
        for copy in weights:
            copy.wait()
        cols = pl.ds(pl.multiple_of(me * tokens, tokens), tokens)
        per = short // (2 * dim)
        heads = [(t, 2 * h * dim) for t in range(dkv_buf.shape[0]) for h in range(per)]
        dk_mine = jnp.concatenate([dkv_buf[t, start:start + dim, cols] for t, start in heads], axis=0)
        dv_mine = jnp.concatenate([dkv_buf[t, start + dim:start + 2 * dim, cols] for t, start in heads], axis=0)
        acc[...] = dot(dk_mine.T, dy_buf[ends[0]:ends[1], :])
        acc[...] += dot(dv_mine.T, dy_buf[ends[1]:, :])
        dqb.relay_far()
        keep_dqb.keep.wait()
        dqb.finish_recvs()
        low = me * tokens < half
        first = pl.multiple_of(jnp.where(low, me * tokens, 0), 128)
        second = pl.multiple_of(jnp.where(low, 0, me * tokens - half), 128)
        from_a = pltpu.make_async_copy(dqa_ref.at[:, pl.ds(first, tokens)], dq_buf, dq_sem)
        from_b = pltpu.make_async_copy(dqb_ref.at[:, pl.ds(second, tokens)], dq_buf, dq_sem)

        @pl.when(low)
        def _():
            from_a.start()

        @pl.when(jnp.logical_not(low))
        def _():
            from_b.start()

        from_a.wait()
        acc[...] += dot(dq_buf[...].T, dy_buf[:ends[0], :])
        d_normed = acc[...].astype(BF16).astype(F32)
        acc[...] = d_normed
        x_f32 = x_ref[...].astype(F32)
        inv_rms = lax.rsqrt(jnp.mean(x_f32 * x_f32, axis=-1, keepdims=True) + NORM_EPS)
        part[...] = jnp.sum(d_normed * (x_f32 * inv_rms), axis=0, keepdims=True)
        dots = jnp.mean(acc[...] * gain_ref[...] * (x_ref[...].astype(F32) * inv_rms), axis=-1, keepdims=True)
        copies = []
        for step in range(1, seq_par):
            copies.append(pltpu.make_async_remote_copy(src_ref=part, dst_ref=slots.at[me], send_sem=gain_send.at[step], recv_sem=gain_recv.at[step], device_id={'sp': lax.rem(me + step, seq_par)}, device_id_type=pl.DeviceIdType.MESH))
            copies[-1].start()
        slots[me] = part[...]
        x_hat = x_ref[...].astype(F32) * inv_rms
        dx_ref[...] = (dyl_ref[...].astype(F32) + inv_rms * (acc[...] * gain_ref[...] - x_hat * dots)).astype(BF16)
        for copy in copies:
            copy.wait_recv()
        total = slots[0]
        for step in range(1, seq_par):
            total = total + slots[step]
        dgain_ref[...] = total
        for copy in copies:
            copy.wait_send()
        dqb.finish_sends()
        dkv.finish_sends()


TILES = 8


def tail_gather(o_all, dy_all, normed_all, dqb_t, dkv_t, dqa_all, wq_t, wk_t, wv_t, x_local, dy_local, gain, dim, seq_par):
    rows, seq = o_all.shape
    d_model = dy_all.shape[1]
    pair_rows = dkv_t.shape[0] * seq_par
    tall = rows // TILES
    short = math.gcd(pair_rows, 256)
    hbm = pl.BlockSpec(memory_space=pl.ANY)
    tokens = x_local.shape[0]
    if wq_t.shape[0] + 2 * wk_t.shape[0] != seq:
        raise ValueError('unsupported shapes')
    whole = lambda shape: pl.BlockSpec(shape, lambda i: (0, 0))
    first = lambda i: (jnp.minimum(i, TILES - 1), 0)
    second = lambda i: (jnp.maximum(i - TILES, 0), 0)
    return pl.pallas_call(
        functools.partial(tail_gather_kernel, seq_par, dim),
        grid=(TILES + pair_rows // short,),
        in_specs=[pl.BlockSpec((tall, seq), first)] + [hbm] * 8 + [whole(x_local.shape), whole(x_local.shape), whole((1, d_model))],
        out_specs=[pl.BlockSpec((tall, d_model), first), pl.BlockSpec((short // 2, d_model), second), pl.BlockSpec((short // 2, d_model), second), hbm, hbm, whole(x_local.shape), whole((1, d_model))],
        out_shape=[
            jax.ShapeDtypeStruct((rows, d_model), F32),
            jax.ShapeDtypeStruct((pair_rows // 2, d_model), F32),
            jax.ShapeDtypeStruct((pair_rows // 2, d_model), F32),
            jax.ShapeDtypeStruct((dqb_t.shape[0] * seq_par, dqb_t.shape[1]), BF16),
            jax.ShapeDtypeStruct((pair_rows, seq), BF16),
            jax.ShapeDtypeStruct(x_local.shape, BF16),
            jax.ShapeDtypeStruct((1, d_model), F32),
        ],
        scratch_shapes=[
            pltpu.VMEM(dy_all.shape, BF16),
            pltpu.VMEM(normed_all.shape, BF16),
            pltpu.VMEM((pair_rows // short, short, seq), BF16),
            pltpu.SemaphoreType.DMA((2,)),
            pltpu.SemaphoreType.DMA((pair_rows // short,)),
            pltpu.VMEM(dqb_t.shape, BF16),
            pltpu.VMEM(dkv_t.shape, BF16),
            pltpu.SemaphoreType.DMA((2,)),
            pltpu.SemaphoreType.DMA((2,)),
        ] + GATHER_SEMS + GATHER_SEMS + [
            pltpu.VMEM((wq_t.shape[0], tokens), BF16),
            pltpu.VMEM((tokens, d_model), F32),
            pltpu.VMEM((1, d_model), F32),
            pltpu.VMEM((seq_par, 1, d_model), F32),
            pltpu.SemaphoreType.DMA((3,)),
            pltpu.SemaphoreType.DMA,
            pltpu.SemaphoreType.DMA((seq_par,)),
            pltpu.SemaphoreType.DMA((seq_par,)),
        ],
        compiler_params=pltpu.CompilerParams(collective_id=5, has_side_effects=True, vmem_limit_bytes=63 << 20),
        cost_estimate=pl.CostEstimate(flops=2 * d_model * seq * (rows + pair_rows), transcendentals=0, bytes_accessed=8 * rows * d_model),
        name='tail_gather',
    )(o_all, dy_all, normed_all, dqb_t, dkv_t, dqa_all, wq_t, wk_t, wv_t, x_local, dy_local, gain[None])


def finish_kernel(dqa_ref, dqb_ref, dwo_in, dk_in, dv_in, y_in, dx_in, r_ref, dwq_ref, dwo_ref, dk_ref, dv_ref, y_ref, dx_ref, r_buf, load_sem):
    half = dqa_ref.shape[1]
    early = pltpu.make_async_copy(r_ref.at[:half, :], r_buf.at[:half, :], load_sem.at[0])
    late = pltpu.make_async_copy(r_ref.at[half:, :], r_buf.at[half:, :], load_sem.at[1])

    @at_step(0)
    def _():
        early.start()
        late.start()

    def hand_on():
        dwo_ref[...] = dwo_in[...]
        dk_ref[...] = dk_in[...]
        dv_ref[...] = dv_in[...]
        y_ref[...] = y_in[...]
        dx_ref[...] = dx_in[...]

    @at_step(0)
    def _():
        hand_on()
        early.wait()
        dwq_ref[...] = dot(dqa_ref[...], r_buf[:half, :])
        late.wait()
        dwq_ref[...] += dot(dqb_ref[...], r_buf[half:, :])

    @pl.when(pl.program_id(0) > 0)
    def _():
        hand_on()
        dwq_ref[...] = dot(dqa_ref[...], r_buf[:half, :]) + dot(dqb_ref[...], r_buf[half:, :])


def finish_grads(dqa_all, dqb_all, passed, normed_all):
    rows, half = dqa_all.shape
    seq, d_model = normed_all.shape
    band = lambda a: pl.BlockSpec((a.shape[0] // TILES, a.shape[1]), lambda i: (i, 0))
    out = jax.ShapeDtypeStruct((rows, d_model), F32)
    return pl.pallas_call(
        finish_kernel,
        grid=(TILES,),
        in_specs=[band(dqa_all), band(dqb_all)] + [band(p) for p in passed] + [pl.BlockSpec(memory_space=pl.ANY)],
        out_specs=[band(out)] + [band(p) for p in passed],
        out_shape=[out] + [jax.ShapeDtypeStruct(p.shape, p.dtype) for p in passed],
        scratch_shapes=[pltpu.VMEM(normed_all.shape, BF16), pltpu.SemaphoreType.DMA((2,))],
        compiler_params=pltpu.CompilerParams(vmem_limit_bytes=60 << 20),
        cost_estimate=pl.CostEstimate(flops=2 * d_model * rows * seq, transcendentals=0, bytes_accessed=16 * rows * d_model),
        name='finish_grads',
    )(dqa_all, dqb_all, *passed, normed_all)


def solution(mesh):
    seq_par = mesh.shape['sp']

    def local_step(x_local, dy_local, gain, w_q, w_k, w_v, w_o):
        _, seq_loc, d_model = x_local.shape
        num_q, dim = w_q.shape[1], w_q.shape[2]
        num_kv = w_k.shape[1]
        group = num_q // num_kv
        if num_kv != seq_par or seq_par % 4:
            raise ValueError('unsupported mesh')
        seq = seq_loc * seq_par
        x_local = x_local[0]
        dy_local = dy_local[0]
        wq_t = jnp.transpose(w_q, (1, 2, 0)).reshape(num_q * dim, d_model)
        wk_t = jnp.transpose(w_k, (1, 2, 0)).reshape(num_kv * dim, d_model)
        wv_t = jnp.transpose(w_v, (1, 2, 0)).reshape(num_kv * dim, d_model)
        wo_t = w_o.reshape(num_q * dim, d_model)

        cos_t, sin_t = rope_tables(jnp.arange(seq, dtype=F32), dim)
        normed_all, q_t, k_t, k_rows, v_rows, o_t, lse, dy_all = attention_forward(x_local, gain, wq_t, wk_t, wv_t, cos_t, sin_t, dy_local, group, seq_par)
        dqb_t, dkv_t, y_out, o_all, dqa_all = attention_backward(x_local, q_t, dy_all, wo_t, o_t, lse, k_rows, v_rows, k_t, cos_t, sin_t, group, seq_par)
        d_wo, d_wk, d_wv, dqb_all, _, d_x, d_gain = tail_gather(o_all, dy_all, normed_all, dqb_t, dkv_t, dqa_all, wq_t, wk_t, wv_t, x_local, dy_local, gain, dim, seq_par)
        d_wq, d_wo, d_wk, d_wv, y_out, d_x = finish_grads(dqa_all, dqb_all, [d_wo, d_wk, d_wv, y_out, d_x], normed_all)
        unflat = lambda g, heads: jnp.transpose(g.reshape(heads, dim, d_model), (2, 0, 1))
        return y_out[None], d_x[None], unflat(d_wq, num_q), unflat(d_wk, num_kv), unflat(d_wv, num_kv), d_wo.reshape(num_q, dim, d_model), d_gain[0]

    specs_in = (P('dp', 'sp', None), P('dp', 'sp', None), P(None), P(None, None, None), P(None, None, None), P(None, None, None), P(None, None, None))
    specs_out = (P('dp', 'sp', None), P('dp', 'sp', None), P('dp', None, None), P('dp', None, None), P('dp', None, None), P('dp', None, None), P('dp'))
    return jax.shard_map(local_step, mesh=mesh, in_specs=specs_in, out_specs=specs_out, check_vma=False)
```
